32 devices in a mesh: row: 4 (over y, x), col: 4 (over z), batch: 2 (over core).
Axes of the slice: x: 2, y: 2, z: 4, core: 2. Of those that a mesh axis runs over, the one named last changes fastest.
Arguments:
- item_ids: int32 [4, 4, 2048], P('batch', 'col', 'row'), parts along dimension 0, may hold values from 0 to 511
- pad_masks: int32 [4, 4, 2048], P('batch', 'col', 'row'), parts along dimension 0, may hold values from 0 to 1
- lengths: int32 [4], P('batch'), parts along dimension 0, may hold values from 7168 to 8192
- item_table: bfloat16 [512, 1024], replicated, may hold values from -5 to 5
- w_gate: bfloat16 [1024, 1024], replicated, may hold values from -0.1875 to 0.1875
- w_in: bfloat16 [1024, 1280], replicated, may hold values from -0.1875 to 0.1875
- w_dt: bfloat16 [1024, 8], replicated, may hold values from -0.1875 to 0.1875
- conv_taps: float32 [4, 1280], replicated, may hold values from -3 to 3
- dt_bias: float32 [8], replicated, may hold values from -2 to 1
- decay_rates: float32 [8], replicated, may hold values from 1.2207031e-05 to 0.05
- norm_gain: float32 [1024], replicated, may hold values from 0.1 to 1.9
- w_out: bfloat16 [1024, 1024], replicated, may hold values from -0.1875 to 0.1875
Outputs:
- result: bfloat16 [4, 4, 2048, 1024], P('batch', 'col', 'row'), parts along dimension 0
The draws below stay inside these ranges and needn't reach their ends.
There are 2 independent parts, one for each index of `batch`. The reference program is written for one: setup_inputs(seed, part) draws one part's arguments, and reference() takes and returns one part's arrays. A program takes and returns all parts, laid end to end along the dimension named above; an argument that names none is the same for every part. Nothing has to cross between parts.
Inputs may be any that keep to these rules, and one draw needn't show every extreme that they name: `lengths`: every history keeps at least its first 7168 positions before padding.
All inputs are finite; a program needn't handle non-finite values.
Results may differ from the reference program's by a relative error of at most 0.0093.
Values may be sent and summed in bfloat16 or wider, within the bound.
A program may use at most 128 MiB of HBM per device.

```python
import math
import jax
import jax.numpy as jnp
import numpy as np
from jax import lax

D = 1024
H = 8
NS = 128
KW = 4
STRETCH = 128
ITEMS = 512
SEQS = 2
TOK_DEV = 512
DI = 1024
BLOCKS = 4
BLOCK_LEN = 2048
LENGTH = 8192


def draw_pad_masks(key, part):
    level_key = jax.random.fold_in(key, 17)
    entry_key = jax.random.fold_in(key, 29)
    spans = BLOCK_LEN // TOK_DEV
    levels = jax.random.randint(level_key, (SEQS, BLOCKS, spans, 1), 1, 5, dtype=jnp.int32)
    entries = jax.random.randint(entry_key, (SEQS, BLOCKS, spans, TOK_DEV), 0, 4, dtype=jnp.int32)
    kept = (entries < levels).astype(jnp.int32)
    return kept.reshape(SEQS, BLOCKS, BLOCK_LEN)


def place_ends(values, key, least, largest):
    dims = values.shape
    spot = [jax.random.randint(jax.random.fold_in(key, axis), (), 0, dims[axis]) for axis in range(len(dims))]
    values = values.at[tuple(spot)].set(least)
    longest = dims.index(max(dims))
    spot[longest] = (spot[longest] + 1) % dims[longest]
    return values.at[tuple(spot)].set(largest)


def cumulative_ranks(number_of, skew):
    loads = [(1 << 20) // math.isqrt(grade ** skew) + 1 for grade in range(1, number_of + 1)]
    deviation = 1 + sum(loads) // (1 << 30)
    return np.cumsum(np.array([max(1, weight // deviation) for weight in loads]))


def ranked_ids(rng, shape, count, skew):
    listing = cumulative_ranks(count, skew)
    lot = jax.random.randint(jax.random.fold_in(rng, 1), shape, 0, int(listing[count - 1]))
    rank = jnp.searchsorted(jnp.asarray(listing, jnp.int32), lot, side="right")
    return jax.random.permutation(jax.random.fold_in(rng, 2), count)[rank].astype(jnp.int32)


def gaussian(rng, extent, width, bound, kind=jnp.bfloat16):
    array = jax.random.normal(rng, extent, jnp.float32) * width
    return jnp.minimum(jnp.maximum(array, -bound), bound).astype(kind)


def setup_inputs(seed: int = 0, part: int = 0) -> dict:
    key_list = jax.random.split(jax.random.key(seed), 13)
    part_keys = jax.random.split(jax.random.fold_in(key_list[12], part), 13)
    return {
        "item_ids": place_ends(ranked_ids(part_keys[0], (SEQS, BLOCKS, BLOCK_LEN), ITEMS, 2), jax.random.fold_in(part_keys[0], 3), 0, ITEMS - 1).astype(jnp.int32),
        "pad_masks": draw_pad_masks(jax.random.fold_in(jax.random.fold_in(key_list[12], part), 71), part),
        "lengths": jax.random.randint(part_keys[2], (SEQS,), LENGTH - BLOCK_LEN // 2, LENGTH + 1).astype(jnp.int32),
        "item_table": gaussian(key_list[3], (ITEMS, D), 1.0, 5.0),
        "w_gate": gaussian(key_list[4], (D, DI), D ** -0.5, 0.1875),
        "w_in": gaussian(key_list[5], (D, DI + 2 * NS), D ** -0.5, 0.1875),
        "w_dt": gaussian(key_list[6], (D, H), D ** -0.5, 0.1875),
        "conv_taps": gaussian(key_list[7], (KW, DI + 2 * NS), 0.5, 3.0, jnp.float32),
        "dt_bias": jnp.clip(jax.random.uniform(key_list[8], (H,), jnp.float32, -2.0, 1.0), -2.0, 1.0),
        "decay_rates": jnp.clip(jnp.exp(jax.random.uniform(key_list[9], (H,), jnp.float32, math.log(1.220703143189894e-05), math.log(0.05))), 1.220703143189894e-05, 0.05),
        "norm_gain": jnp.clip(1.0 + 0.18 * jax.random.normal(key_list[10], (DI,), jnp.float32), 0.1, 1.9),
        "w_out": gaussian(key_list[11], (DI, D), DI ** -0.5, 0.1875),
    }


def rounded(value):
    return lax.optimization_barrier(value.astype(jnp.bfloat16)).astype(jnp.float32)

def reference(item_ids, pad_masks, lengths, item_table, w_gate, w_in, w_dt, conv_taps, dt_bias, decay_rates, norm_gain, w_out):
    users = item_ids.shape[0]
    events = item_ids.shape[1] * item_ids.shape[2]
    stretch_count = events // STRETCH
    full_width = w_in.shape[1]
    inner_width = w_gate.shape[1]
    head_count = decay_rates.shape[0]
    head_size = inner_width // head_count
    state_width = (full_width - inner_width) // 2
    kernel = conv_taps.shape[0]
    item_stretches = item_ids.reshape(users, stretch_count, STRETCH).transpose(1, 0, 2)
    mask_stretches = pad_masks.reshape(users, stretch_count, STRETCH).transpose(1, 0, 2)
    starts = jnp.arange(stretch_count, dtype=jnp.int32) * STRETCH
    within = jnp.arange(STRETCH, dtype=jnp.int32)
    causal = within[:, None] >= within[None, :]

    def advance(carried, inputs):
        state_now, before = carried
        item_rows, mask_rows, start = inputs
        embedded = jnp.take(item_table, item_rows, axis=0).reshape(users * STRETCH, -1)
        projected = jnp.dot(embedded, w_in, preferred_element_type=jnp.float32).astype(jnp.bfloat16).reshape(users, STRETCH, full_width)
        gate_rows = rounded(jnp.dot(embedded, w_gate, preferred_element_type=jnp.float32)).reshape(users, STRETCH, inner_width)
        step_raw = jnp.dot(embedded, w_dt, preferred_element_type=jnp.float32).reshape(users, STRETCH, head_count)
        joined = lax.optimization_barrier(jnp.concatenate([before, projected], axis=1)).astype(jnp.float32)
        convolved = joined[:, 0:STRETCH, :] * conv_taps[0]
        for offset in range(1, kernel):
            convolved = convolved + joined[:, offset:offset + STRETCH, :] * conv_taps[offset]
        signal = rounded(jax.nn.silu(convolved[..., :inner_width]))
        inward = rounded(convolved[..., inner_width:inner_width + state_width])
        outward = rounded(convolved[..., inner_width + state_width:])
        position = start + within
        usable = jnp.logical_and(position[None, :] < lengths[:, None], mask_rows > 0).astype(jnp.float32)
        step_size = usable[..., None] * jax.nn.softplus(step_raw + dt_bias)
        log_decay = jnp.cumsum(step_size * decay_rates, axis=1)
        log_heads = log_decay.transpose(0, 2, 1)
        size_heads = step_size.transpose(0, 2, 1)
        scores = jnp.einsum('sqn,sun->squ', outward, inward)
        log_gap = log_heads[:, :, :, None] - log_heads[:, :, None, :]
        decays = jnp.where(causal, jnp.exp(-jnp.where(causal, log_gap, 0.0)), 0.0)
        weights = rounded(scores[:, None] * decays * size_heads[:, :, None, :])
        signal_heads = signal.reshape(users, STRETCH, head_count, head_size)
        local_out = jnp.einsum('shqu,suhp->sqhp', weights, signal_heads)
        entering = rounded(state_now)
        carried_out = jnp.einsum('sqn,shpn->sqhp', outward, entering) * jnp.exp(-log_decay)[..., None]
        mixture = (local_out + carried_out).reshape(users, STRETCH, inner_width)
        gated_rows = mixture * jax.nn.silu(gate_rows)
        normed = (gated_rows * lax.rsqrt(lax.optimization_barrier(jnp.mean(gated_rows * gated_rows, axis=-1, keepdims=True)) + 1.0) * norm_gain).astype(jnp.bfloat16)
        result = jnp.dot(normed.reshape(users * STRETCH, inner_width), w_out, preferred_element_type=jnp.float32).reshape(users, STRETCH, -1)
        result = (result * usable[..., None]).astype(jnp.bfloat16)
        tail_weight = jnp.exp(log_heads - log_heads[:, :, -1:]) * size_heads
        scaled_in = rounded(inward[:, None, :, :] * tail_weight[..., None])
        stretch_state = jnp.einsum('shun,suhp->shpn', scaled_in, signal_heads)
        new_state = jnp.exp(-log_heads[:, :, -1])[..., None, None] * state_now + stretch_state
        return ((new_state, projected[:, STRETCH - (kernel - 1):, :]), result)
    initial = (jnp.zeros((users, head_count, head_size, state_width), jnp.float32), jnp.zeros((users, kernel - 1, full_width), jnp.bfloat16))
    _, results = lax.scan(advance, initial, (item_stretches, mask_stretches, starts))
    return results.transpose(1, 0, 2, 3).reshape(item_ids.shape + (item_table.shape[1],))
```

```python
import functools

import jax
import jax.numpy as jnp
from jax import lax
from jax.experimental import pallas as pl
from jax.experimental.pallas import tpu as pltpu
from jax.sharding import PartitionSpec as P

STRETCH = 128
LANES = 128
HALO = 16
MESH = pl.DeviceIdType.MESH
F32 = jnp.float32
BF16 = jnp.bfloat16


def silu(v):
    return 0.5 * v * (1.0 + jnp.tanh(0.5 * v))


def remote(src, dst, send, recv, device):
    return pltpu.make_async_remote_copy(
        src_ref=src,
        dst_ref=dst,
        send_sem=send,
        recv_sem=recv,
        device_id=device,
        device_id_type=MESH,
    )


def mixer_kernel(
    counts,
    lengths_ref,
    ids_ref,
    masks_ref,
    wdt_ref,
    taps_ref,
    bias_ref,
    rates_ref,
    gain_ref,
    table_hbm,
    win_hbm,
    wgate_hbm,
    wout_hbm,
    out_ref,
    table,
    win,
    wgate,
    wout,
    tin,
    tgate,
    tdt,
    wide,
    params,
    ptaps,
    hot,
    rowbuf,
    inward_t,
    outward,
    logs,
    logs_t,
    steps_t,
    tails,
    shrinks,
    ef,
    signal,
    scaled,
    held,
    ssend,
    rin,
    aft,
    lin,
    before,
    pin,
    psend,
    esend,
    enter,
    y,
    gates,
    mix,
    ostage,
    landed,
    wsem,
    osem,
    hsem,
    ssem,
    lsem_s,
    lsem_r,
    s1,
    r1,
    s2,
    r2,
    s3,
    r3,
):
    rows, cols, users, heads, tall = counts
    events = ids_ref.shape[2]
    stretches = events // STRETCH
    kernel = taps_ref.shape[0]
    inner = wgate.shape[1]
    per = heads // rows
    pieces = users * per
    wide_group = rows * LANES
    r, c = lax.axis_index("row"), lax.axis_index("col")
    place = c * rows + r
    places = rows * cols
    later = lax.rem(place + 1, places)
    earlier = lax.rem(place + places - 1, places)
    after = {"row": lax.rem(later, rows), "col": later // rows}
    ahead = {"row": lax.rem(earlier, rows), "col": earlier // rows}
    has_after, has_before = place < places - 1, place > 0
    wraps = jnp.logical_and(r == rows - 1, c < cols - 1)
    wrapped = jnp.logical_and(r == 0, c > 0)

    def head_of(p):
        return (p % rows) * per + p // rows

    def column(p):
        source = p if p >= heads else head_of(p)
        return pltpu.make_async_copy(
            win_hbm.at[:, pl.ds(source * LANES, LANES)],
            win.at[:, pl.ds(p * LANES, LANES)],
            wsem.at[p],
        )

    blocks = heads + 2
    table_copy = pltpu.make_async_copy(table_hbm, table, wsem.at[blocks])
    wgate_copy = pltpu.make_async_copy(wgate_hbm, wgate, wsem.at[blocks + 1])
    wout_copy = pltpu.make_async_copy(wout_hbm, wout, wsem.at[blocks + 2])
    table_copy.start()
    for p in (heads, heads + 1, *range(heads)):
        column(p).start()
    wgate_copy.start()
    wout_copy.start()

    barrier = pltpu.get_barrier_semaphore()
    for d in range(1, rows):
        pl.semaphore_signal(
            barrier, inc=1, device_id={"row": lax.rem(r + d, rows)}, device_id_type=MESH
        )

    @pl.when(c > 0)
    def _():
        pl.semaphore_signal(barrier, inc=1, device_id={"col": c - 1}, device_id_type=MESH)

    @pl.when(c < cols - 1)
    def _():
        pl.semaphore_signal(barrier, inc=1, device_id={"col": c + 1}, device_id_type=MESH)

    @pl.when(wraps)
    def _():
        pl.semaphore_signal(barrier, inc=1, device_id=after, device_id_type=MESH)

    @pl.when(wrapped)
    def _():
        pl.semaphore_signal(barrier, inc=1, device_id=ahead, device_id_type=MESH)

    halo_copy = remote(
        ids_ref.at[:, :, pl.ds(events - STRETCH, STRETCH)], landed, hsem.at[0], hsem.at[1], after
    )

    params[...] = jnp.zeros_like(params)
    wide[...] = jnp.zeros_like(wide)
    for p in range(heads):
        h = head_of(p)
        params[0:1, p : p + 1] = bias_ref[:, h : h + 1]
        params[1:2, p : p + 1] = rates_ref[:, h : h + 1]
    wide[0:heads, :] = jnp.concatenate(
        [wdt_ref[head_of(p) : head_of(p) + 1, :] for p in range(heads)], axis=0
    )
    for p in range(blocks):
        source = p if p >= heads else head_of(p)
        ptaps[p, 0:kernel, :] = taps_ref[:, source * LANES : (source + 1) * LANES]

    table_copy.wait()

    def table_block(first):
        span = pl.ds(first, 2 * LANES)
        if not isinstance(first, int):
            span = pl.ds(pl.multiple_of(first, 2 * LANES), 2 * LANES)
        tin[:, span] = jnp.dot(table[...], win[:, span], preferred_element_type=F32).astype(BF16)

    column(heads).wait()
    column(heads + 1).wait()
    table_block(heads * LANES)

    peers = (
        rows
        - 1
        + jnp.where(c > 0, 1, 0)
        + jnp.where(c < cols - 1, 1, 0)
        + jnp.where(wraps, 1, 0)
        + jnp.where(wrapped, 1, 0)
    )
    pl.semaphore_wait(barrier, peers)

    @pl.when(has_after)
    def _():
        halo_copy.start()

    raw = lax.dot_general(
        table[...], wide[...], (((1,), (1,)), ((), ())), preferred_element_type=F32
    )
    high = raw.astype(BF16).astype(F32)
    middle = (raw - high).astype(BF16).astype(F32)
    low = raw - high - middle
    tdt[...] = (high + pltpu.roll(middle, heads, 1) + pltpu.roll(low, 2 * heads, 1)).astype(BF16)

    for p in range(heads):
        column(p).wait()

    def table_step(i, carry):
        table_block(i * 2 * LANES)
        return carry

    lax.fori_loop(0, heads // 2, table_step, 0)

    @pl.when(place == 0)
    def _():
        landed[...] = jnp.full(landed.shape, -1, jnp.int32)

    @pl.when(has_before)
    def _():
        halo_copy.wait_recv()

    line_rows = lax.broadcasted_iota(jnp.int32, (STRETCH, STRETCH), 0)
    line_cols = lax.broadcasted_iota(jnp.int32, (STRETCH, STRETCH), 1)
    causal = line_rows >= line_cols

    def convolve(position, slot):
        total = None
        for k in range(kernel):
            part = rowbuf[slot, pl.ds(HALO - kernel + 1 + k, events), :] * ptaps[position, k : k + 1, :]
            total = part if total is None else total + part
        return total

    def log_copy(u, d):
        q = lax.rem(r + d, rows)
        return remote(
            aft.at[u, q], lin.at[u, r], lsem_s.at[u, d], lsem_r.at[u, d], {"row": q}
        )

    def state_copy(k, d):
        q = lax.rem(r + d, rows)
        return remote(ssend.at[k, q], rin.at[k, r], s1.at[k, d], r1.at[k, d], {"row": q})

    def onward_copy(k):
        return remote(
            psend.at[k], pin.at[k], s2.at[k], r2.at[k], {"col": lax.rem(c + 1, cols)}
        )

    def enter_copy(k, d):
        q = lax.rem(r + d, rows)
        return remote(esend.at[k, q], enter.at[k, r], s3.at[k, d], r3.at[k, d], {"row": q})

    def prepare(u):
        first = place * events
        names = jnp.concatenate([landed[u], ids_ref[u]], axis=1).astype(F32)
        position = first + lax.broadcasted_iota(jnp.int32, (1, events), 1)
        kept = jnp.where(position < lengths_ref[u], masks_ref[u], 0)
        kept = jnp.where(kept > 0, 1.0, 0.0).astype(F32)
        flags = jnp.concatenate([jnp.zeros((1, STRETCH), F32), kept], axis=1)
        line = lax.broadcasted_iota(jnp.int32, (8, STRETCH + events), 0)
        meta = jnp.transpose(jnp.where(line == 0, names, jnp.where(line == 1, flags, 0.0)))
        usable = meta[STRETCH:, 1:2]
        ids = meta[STRETCH - HALO :, 0:1].astype(jnp.int32)
        items = table.shape[0]
        lane = lax.broadcasted_iota(jnp.int32, (HALO + events, items), 1)
        hot[u] = (ids == lane).astype(F32).astype(BF16)
        both = jnp.dot(hot[u], tin[:, heads * LANES :], preferred_element_type=F32)
        rowbuf[0] = both[:, :LANES]
        rowbuf[1] = both[:, LANES:]
        parts = jnp.dot(hot[u, pl.ds(HALO, events), :], tdt[...], preferred_element_type=F32)
        raw = (
            parts
            + pltpu.roll(parts, LANES - heads, 1)
            + pltpu.roll(parts, LANES - 2 * heads, 1)
        )
        raw = raw + params[0:1, :]
        step = usable * (jnp.maximum(raw, 0.0) + jnp.log1p(jnp.exp(-jnp.abs(raw))))
        paced = step * params[1:2, :]
        inward_t[u] = jnp.transpose(convolve(heads, 0)).astype(BF16)
        outward[pl.ds(pl.multiple_of(u * events, events), events), :] = convolve(heads + 1, 1).astype(BF16)
        past = jnp.zeros((1, LANES), F32)
        lower = jnp.where(causal, 1.0, 0.0).astype(F32)
        for s in range(stretches):
            span = slice(s * STRETCH, (s + 1) * STRETCH)
            log = jnp.dot(
                lower, paced[span], precision=lax.Precision.HIGHEST, preferred_element_type=F32
            )
            logs[u, span, :] = log
            logs_t[u, s] = jnp.transpose(log)[0:8, :]
            steps_t[u, s] = jnp.transpose(step[span])[0:8, :]
            total = log[STRETCH - 1 :, :]
            tail = jnp.exp(log - total) * step[span]
            shrink = jnp.exp(-total)
            for j in range(per):
                turned = tail if j == 0 else pltpu.roll(tail, LANES - j * rows, 1)
                tails[u * per + j, span, :] = turned
                for q in range(rows):
                    p = j * rows + q
                    shrinks[u * per + j, s, :, q * LANES : (q + 1) * LANES] = jnp.broadcast_to(
                        shrink[:, p : p + 1], (8, LANES)
                    )
            lane = lax.broadcasted_iota(jnp.int32, (STRETCH, LANES), 1)
            ef[pl.ds(pl.multiple_of(u * events + s * STRETCH, STRETCH), STRETCH), :] = jnp.where(
                lane == LANES - 1, usable[span], jnp.exp(-(log + past))
            )
            past = past + total
        for q in range(rows):
            for j in range(per):
                p = j * rows + q
                aft[u, q, j] = jnp.broadcast_to(past[:, p : p + 1], (8, LANES))
        for d in range(1, rows):
            log_copy(u, d).start()
        lin[u, r] = aft[u, r]

    def group(u, j):
        k = u * per + j
        base = pl.multiple_of(j * wide_group, wide_group)
        gathered = jnp.dot(hot[u], tin[:, pl.ds(base, wide_group)], preferred_element_type=F32)
        for q in range(rows):
            rowbuf[q] = gathered[:, q * LANES : (q + 1) * LANES]
        for q in range(rows):
            span = slice(q * LANES, (q + 1) * LANES)
            value = silu(convolve(j * rows + q, q)).astype(BF16)
            signal[u, j * rows + q] = value
            scaled[:, span] = (value.astype(F32) * tails[k, :, q : q + 1]).astype(BF16)
        run = None
        for s in range(stretches):
            span = slice(s * STRETCH, (s + 1) * STRETCH)
            added = jnp.dot(
                inward_t[u, :, span], scaled[span, :], preferred_element_type=F32
            )
            if run is None:
                held[k, s] = jnp.zeros_like(held[k, s])
                run = added
            else:
                held[k, s] = run.astype(BF16)
                run = run * shrinks[k, s, 0:1, :] + added
        for q in range(rows):
            ssend[k, q] = run[:, q * LANES : (q + 1) * LANES].astype(BF16)
        for d in range(1, rows):
            state_copy(k, d).start()

    def user_step(u, carry):
        prepare(u)

        def group_step(j, inner_carry):
            group(u, j)
            return inner_carry

        return lax.fori_loop(0, per, group_step, carry)

    lax.fori_loop(0, users, user_step, 0)

    def handle(k, carry):
        u, j = k // per, lax.rem(k, per)
        rin[k, r] = ssend[k, r]

        @pl.when(j == 0)
        def _():
            for d in range(1, rows):
                log_copy(u, d).wait_recv()

        for d in range(1, rows):
            state_copy(k, d).wait_recv()
        carried = jnp.zeros(pin.shape[1:], F32)
        fade = jnp.ones((1, LANES), F32)
        fades = []
        for m in range(rows):
            before[m] = carried
            fades.append(fade)
            here = jnp.exp(-lin[u, m, j, 0:1, :])
            carried = here * carried + rin[k, m].astype(F32)
            fade = fade * here

        @pl.when(c == 0)
        def _():
            pin[k] = jnp.zeros(pin.shape[1:], BF16)
            psend[k] = carried.astype(BF16)
            if cols > 1:
                onward_copy(k).start()

        if cols > 1:

            @pl.when(c > 0)
            def _():
                onward_copy(k).wait_recv()

            @pl.when(jnp.logical_and(c > 0, c < cols - 1))
            def _():
                psend[k] = (fade * pin[k].astype(F32) + carried).astype(BF16)
                onward_copy(k).start()

        for q in range(rows):
            esend[k, q] = (fades[q] * pin[k].astype(F32) + before[q]).astype(BF16)
        for d in range(1, rows):
            enter_copy(k, d).start()
        enter[k, r] = esend[k, r]
        return carry

    ticks = users * stretches

    def due(t):
        reach = (2 * t + 1 - 4 * c + 3 * 4 * cols) // 3 - 4 * cols + 1
        return jnp.minimum(jnp.maximum(reach, 0), pieces)

    wgate_copy.wait()
    chunk = inner // stretches

    def local_step(t, done):
        now = due(t)
        lax.fori_loop(done, now, handle, 0)
        u, s = t // stretches, lax.rem(t, stretches)
        span = pl.ds(pl.multiple_of(s * chunk, chunk), chunk)
        mine = pl.ds(pl.multiple_of(u * events, events), events)

        @pl.when(u == 0)
        def _():
            tgate[:, span] = jnp.dot(
                table[...], wgate[:, span], preferred_element_type=F32
            ).astype(BF16)

        gates[mine, span] = silu(
            jnp.dot(hot[u, pl.ds(HALO, events), :], tgate[:, span], preferred_element_type=F32)
        )
        base = pl.multiple_of(s * STRETCH, STRETCH)
        place_rows = pl.ds(pl.multiple_of(u * events + s * STRETCH, STRETCH), STRETCH)
        seen = outward[place_rows, :]
        scores = jnp.dot(
            seen, inward_t[u, :, pl.ds(base, STRETCH)], preferred_element_type=F32
        )
        scores = jnp.where(causal, scores, 0.0)
        log = logs[u, pl.ds(base, STRETCH), :]
        fade = jnp.exp(-log)
        wide_seen = seen.astype(F32)
        for p in range(heads):
            h = head_of(p)
            gap = jnp.minimum(logs_t[u, s, p : p + 1, :] - log[:, p : p + 1], 0.0)
            weights = (jnp.exp(gap) * (scores * steps_t[u, s, p : p + 1, :])).astype(BF16)
            faded = (wide_seen * fade[:, p : p + 1]).astype(BF16)
            q = p % rows
            right = jnp.concatenate(
                [
                    signal[u, p, pl.ds(base, STRETCH), :],
                    held[u * per + p // rows, s, :, q * LANES : (q + 1) * LANES],
                ],
                axis=0,
            )
            y[place_rows, h * LANES : (h + 1) * LANES] = jnp.dot(
                jnp.concatenate([weights, faded], axis=1), right, preferred_element_type=F32
            )
        return now

    done = lax.fori_loop(0, ticks, local_step, 0)
    lax.fori_loop(done, pieces, handle, 0)
    wout_copy.wait()
    tiles = events // tall

    def out_copy(i):
        span = pl.ds(pl.multiple_of(i * tall, tall), tall)
        return pltpu.make_async_copy(ostage.at[span, :], out_ref.at[span, :], osem.at[i])

    def finish_step(i, carry):
        u = i // tiles

        @pl.when(lax.rem(i, tiles) == 0)
        def _():
            for j in range(per):
                for d in range(1, rows):
                    enter_copy(u * per + j, d).wait_recv()

        span = pl.ds(pl.multiple_of(i * tall, tall), tall)
        squares = None
        for p in range(0, heads, 2):
            far = jnp.dot(
                outward[span, :],
                jnp.concatenate(
                    [enter[u * per + e // rows, e % rows] for e in (p, p + 1)], axis=1
                ),
                preferred_element_type=F32,
            )
            for e in (p, p + 1):
                h = head_of(e)
                where = slice(h * LANES, (h + 1) * LANES)
                part = far[:, (e - p) * LANES : (e - p + 1) * LANES]
                value = (y[span, where] + part * ef[span, e : e + 1]) * gates[span, where]
                mix[:, where] = value
                squares = value * value if squares is None else squares + value * value
        mean = jnp.sum(squares, axis=1, keepdims=True) * (1.0 / inner)
        normed = (mix[...] * lax.rsqrt(mean + 1.0) * gain_ref[...]).astype(BF16)
        result = jnp.dot(normed, wout[...], preferred_element_type=F32)
        ostage[span, :] = (result * ef[span, LANES - 1 : LANES]).astype(BF16)
        out_copy(i).start()
        return carry

    lax.fori_loop(0, users * tiles, finish_step, 0)

    @pl.when(has_after)
    def _():
        halo_copy.wait_send()

    for u in range(users):
        for d in range(1, rows):
            log_copy(u, d).wait_send()
    for k in range(pieces):
        for d in range(1, rows):
            state_copy(k, d).wait_send()
            enter_copy(k, d).wait_send()
    if cols > 1:

        @pl.when(c < cols - 1)
        def _():
            for k in range(pieces):
                onward_copy(k).wait_send()

    for i in range(users * tiles):
        out_copy(i).wait()


def per_device(
    item_ids,
    pad_masks,
    lengths,
    item_table,
    w_gate,
    w_in,
    w_dt,
    conv_taps,
    dt_bias,
    decay_rates,
    norm_gain,
    w_out,
):
    users, _, events = item_ids.shape
    items, model = item_table.shape
    full_width = w_in.shape[1]
    inner = w_gate.shape[1]
    heads = decay_rates.shape[0]
    state_width = (full_width - inner) // 2
    rows, cols = lax.axis_size("row"), lax.axis_size("col")
    stretches = events // STRETCH
    per = heads // rows
    pieces = users * per
    total = users * events
    tall = 2 * STRETCH if events % (2 * STRETCH) == 0 else STRETCH
    group = rows * LANES
    head = (state_width, LANES)

    vmem = pl.BlockSpec(memory_space=pltpu.VMEM)
    hbm = pl.BlockSpec(memory_space=pl.ANY)
    dma = pltpu.SemaphoreType.DMA

    def f32(*shape):
        return pltpu.VMEM(shape, F32)

    def bf16(*shape):
        return pltpu.VMEM(shape, BF16)

    result = pl.pallas_call(
        functools.partial(mixer_kernel, (rows, cols, users, heads, tall)),
        in_specs=[pl.BlockSpec(memory_space=pltpu.SMEM)] + [vmem] * 7 + [hbm] * 4,
        out_specs=hbm,
        out_shape=jax.ShapeDtypeStruct((total, w_out.shape[1]), BF16),
        scratch_shapes=[
            bf16(items, model),
            bf16(model, full_width),
            bf16(model, inner),
            bf16(*w_out.shape),
            bf16(items, full_width),
            bf16(items, inner),
            bf16(items, LANES),
            bf16(LANES, model),
            f32(8, LANES),
            f32(heads + 2, 8, LANES),
            bf16(users, HALO + events, items),
            f32(max(rows, 2), HALO + events, LANES),
            bf16(users, state_width, events),
            bf16(total, state_width),
            f32(users, events, LANES),
            f32(users, stretches, 8, LANES),
            f32(users, stretches, 8, LANES),
            f32(pieces, events, LANES),
            f32(pieces, stretches, 8, group),
            f32(total, LANES),
            bf16(users, heads, events, LANES),
            bf16(events, group),
            bf16(pieces, stretches, state_width, group),
            bf16(pieces, rows, *head),
            bf16(pieces, rows, *head),
            f32(users, rows, per, 8, LANES),
            f32(users, rows, per, 8, LANES),
            f32(rows, *head),
            bf16(pieces, *head),
            bf16(pieces, *head),
            bf16(pieces, rows, *head),
            bf16(pieces, rows, *head),
            f32(total, inner),
            f32(total, inner),
            f32(tall, inner),
            bf16(total, w_out.shape[1]),
            pltpu.VMEM((users, 1, STRETCH), jnp.int32),
            dma((heads + 5,)),
            dma((total // tall,)),
            dma((2,)),
            dma((1,)),
            dma((users, rows)),
            dma((users, rows)),
            dma((pieces, rows)),
            dma((pieces, rows)),
            dma((pieces,)),
            dma((pieces,)),
            dma((pieces, rows)),
            dma((pieces, rows)),
        ],
        compiler_params=pltpu.CompilerParams(
            collective_id=0, has_side_effects=True, vmem_limit_bytes=56 * 1024 * 1024
        ),
        name="mixer",
    )(
        lengths,
        item_ids,
        pad_masks,
        w_dt.T,
        conv_taps,
        dt_bias[None],
        decay_rates[None],
        norm_gain[None],
        item_table,
        w_in,
        w_gate,
        w_out,
    )
    return result.reshape(users, 1, events, -1)


def solution(mesh):
    in_specs = (
        P("batch", "col", "row"),
        P("batch", "col", "row"),
        P("batch"),
        P(),
        P(),
        P(),
        P(),
        P(),
        P(),
        P(),
        P(),
        P(),
    )
    out_specs = P("batch", "col", "row", None)
    return jax.shard_map(
        per_device, mesh=mesh, in_specs=in_specs, out_specs=out_specs, check_vma=False
    )
```

```python
import functools

import jax
import jax.numpy as jnp
from jax import lax
from jax.experimental import pallas as pl
from jax.experimental.pallas import tpu as pltpu
from jax.sharding import PartitionSpec as P

STRETCH = 128
LANES = 128
HALO = 16
MESH = pl.DeviceIdType.MESH
F32 = jnp.float32
BF16 = jnp.bfloat16


def silu(v):
    return 0.5 * v * (1.0 + jnp.tanh(0.5 * v))


def remote(src, dst, send, recv, device):
    return pltpu.make_async_remote_copy(
        src_ref=src,
        dst_ref=dst,
        send_sem=send,
        recv_sem=recv,
        device_id=device,
        device_id_type=MESH,
    )


def mixer_kernel(
    counts,
    lengths_hbm,
    ids_hbm,
    masks_hbm,
    wdt_hbm,
    taps_hbm,
    bias_hbm,
    rates_hbm,
    gain_hbm,
    table_hbm,
    win_hbm,
    wgate_hbm,
    wout_hbm,
    out_ref,
    lengths_ref,
    ids_ref,
    masks_ref,
    wdt_ref,
    taps_ref,
    bias_ref,
    rates_ref,
    gain_ref,
    table,
    win,
    wgate,
    wout,
    tin,
    tgate,
    tdt,
    wide,
    params,
    ptaps,
    hot,
    rowbuf,
    inward_t,
    outward,
    facts,
    logs_t,
    steps_t,
    shrinks,
    signal,
    scaled,
    held,
    ssend,
    rin,
    aft,
    lin,
    before,
    pin,
    psend,
    esend,
    enter,
    y,
    gates,
    mix,
    landed,
    wsem,
    psem,
    hsem,
    lsem_s,
    lsem_r,
    s1,
    r1,
    s2,
    r2,
    s3,
    r3,
):
    rows, cols, users, heads, tall = counts
    events = ids_ref.shape[2]
    stretches = events // STRETCH
    kernel = taps_ref.shape[0]
    inner = wgate.shape[1]
    per = heads // rows
    pieces = users * per
    wide_group = rows * LANES
    r, c = lax.axis_index("row"), lax.axis_index("col")
    place = c * rows + r
    places = rows * cols
    later = lax.rem(place + 1, places)
    earlier = lax.rem(place + places - 1, places)
    after = {"row": lax.rem(later, rows), "col": later // rows}
    ahead = {"row": lax.rem(earlier, rows), "col": earlier // rows}
    has_after, has_before = place < places - 1, place > 0
    wraps = jnp.logical_and(r == rows - 1, c < cols - 1)
    wrapped = jnp.logical_and(r == 0, c > 0)

    def head_of(p):
        return (p % rows) * per + p // rows

    def column(p):
        source = p if p >= heads else head_of(p)
        return pltpu.make_async_copy(
            win_hbm.at[:, pl.ds(source * LANES, LANES)],
            win.at[:, pl.ds(p * LANES, LANES)],
            wsem.at[p],
        )

    blocks = heads + 2
    table_copy = pltpu.make_async_copy(table_hbm, table, wsem.at[blocks])
    wgate_copy = pltpu.make_async_copy(wgate_hbm, wgate, wsem.at[blocks + 1])
    wout_copy = pltpu.make_async_copy(wout_hbm, wout, wsem.at[blocks + 2])
    small = [
        pltpu.make_async_copy(source, target, psem.at[i])
        for i, (source, target) in enumerate(
            (
                (ids_hbm, ids_ref),
                (masks_hbm, masks_ref),
                (lengths_hbm, lengths_ref),
                (wdt_hbm, wdt_ref),
                (taps_hbm, taps_ref),
                (bias_hbm, bias_ref),
                (rates_hbm, rates_ref),
                (gain_hbm, gain_ref),
            )
        )
    ]
    table_copy.start()
    for copy in small:
        copy.start()
    for p in (heads, heads + 1, *range(heads)):
        column(p).start()
    wgate_copy.start()
    wout_copy.start()

    barrier = pltpu.get_barrier_semaphore()
    for d in range(1, rows):
        pl.semaphore_signal(
            barrier, inc=1, device_id={"row": lax.rem(r + d, rows)}, device_id_type=MESH
        )

    @pl.when(c > 0)
    def _():
        pl.semaphore_signal(barrier, inc=1, device_id={"col": c - 1}, device_id_type=MESH)

    @pl.when(c < cols - 1)
    def _():
        pl.semaphore_signal(barrier, inc=1, device_id={"col": c + 1}, device_id_type=MESH)

    @pl.when(wraps)
    def _():
        pl.semaphore_signal(barrier, inc=1, device_id=after, device_id_type=MESH)

    @pl.when(wrapped)
    def _():
        pl.semaphore_signal(barrier, inc=1, device_id=ahead, device_id_type=MESH)

    halo_copy = remote(
        ids_ref.at[:, :, pl.ds(events - STRETCH, STRETCH)], landed, hsem.at[0], hsem.at[1], after
    )

    wide[...] = jnp.zeros_like(wide)
    for copy in small:
        copy.wait()
    line_rows = lax.broadcasted_iota(jnp.int32, (STRETCH, STRETCH), 0)
    line_cols = lax.broadcasted_iota(jnp.int32, (STRETCH, STRETCH), 1)
    causal = line_rows >= line_cols
    for i, source in enumerate((bias_ref, rates_ref)):
        value = jnp.zeros((heads, LANES), F32)
        for p in range(heads):
            value = jnp.where(line_rows[0:heads] == p, source[:, head_of(p) : head_of(p) + 1], value)
        params[i] = value
    wide[0:heads, :] = jnp.concatenate(
        [wdt_ref[head_of(p) : head_of(p) + 1, :] for p in range(heads)], axis=0
    )
    for p in range(blocks):
        source = p if p >= heads else head_of(p)
        ptaps[p, 0:kernel, :] = taps_ref[:, source * LANES : (source + 1) * LANES]

    table_copy.wait()

    def table_block(first):
        span = pl.ds(first, 2 * LANES)
        if not isinstance(first, int):
            span = pl.ds(pl.multiple_of(first, 2 * LANES), 2 * LANES)
        tin[:, span] = jnp.dot(table[...], win[:, span], preferred_element_type=F32).astype(BF16)

    column(heads).wait()
    column(heads + 1).wait()
    table_block(heads * LANES)

    raw = lax.dot_general(
        table[...], wide[...], (((1,), (1,)), ((), ())), preferred_element_type=F32
    )
    high = raw.astype(BF16).astype(F32)
    middle = (raw - high).astype(BF16).astype(F32)
    low = raw - high - middle
    tdt[...] = (high + pltpu.roll(middle, heads, 1) + pltpu.roll(low, 2 * heads, 1)).astype(BF16)

    peers = (
        rows
        - 1
        + jnp.where(c > 0, 1, 0)
        + jnp.where(c < cols - 1, 1, 0)
        + jnp.where(wraps, 1, 0)
        + jnp.where(wrapped, 1, 0)
    )
    pl.semaphore_wait(barrier, peers)

    @pl.when(has_after)
    def _():
        halo_copy.start()

    for p in range(heads):
        column(p).wait()

    def table_step(i, carry):
        table_block(i * 2 * LANES)
        return carry

    lax.fori_loop(0, heads // 2, table_step, 0)
    wgate_copy.wait()

    def gate_step(i, carry):
        span = pl.ds(pl.multiple_of(i * 2 * LANES, 2 * LANES), 2 * LANES)
        tgate[:, span] = jnp.dot(
            table[...], wgate[:, span], preferred_element_type=F32
        ).astype(BF16)
        return carry

    lax.fori_loop(0, inner // (2 * LANES), gate_step, 0)

    @pl.when(place == 0)
    def _():
        landed[...] = jnp.full(landed.shape, -1, jnp.int32)

    @pl.when(has_before)
    def _():
        halo_copy.wait_recv()

    def convolve(position, slot):
        total = None
        for k in range(kernel):
            part = rowbuf[slot, pl.ds(HALO - kernel + 1 + k, events), :] * ptaps[position, k : k + 1, :]
            total = part if total is None else total + part
        return total

    def log_copy(u, d):
        q = lax.rem(r + d, rows)
        return remote(
            aft.at[u, q], lin.at[u, r], lsem_s.at[u, d], lsem_r.at[u, d], {"row": q}
        )

    def state_copy(k, d):
        q = lax.rem(r + d, rows)
        return remote(ssend.at[k, q], rin.at[k, r], s1.at[k, d], r1.at[k, d], {"row": q})

    def onward_copy(k):
        return remote(
            psend.at[k], pin.at[k], s2.at[k], r2.at[k], {"col": lax.rem(c + 1, cols)}
        )

    def enter_copy(k, d):
        q = lax.rem(r + d, rows)
        return remote(esend.at[k, q], enter.at[k, r], s3.at[k, d], r3.at[k, d], {"row": q})

    def prepare(u):
        first = place * events
        names = jnp.concatenate([landed[u], ids_ref[u]], axis=1).astype(F32)
        position = first + lax.broadcasted_iota(jnp.int32, (1, events), 1)
        kept = jnp.where(position < lengths_ref[u], masks_ref[u], 0)
        kept = jnp.where(kept > 0, 1.0, 0.0).astype(F32)
        flags = jnp.concatenate([jnp.zeros((1, STRETCH), F32), kept], axis=1)
        line = lax.broadcasted_iota(jnp.int32, (8, STRETCH + events), 0)
        meta = jnp.transpose(jnp.where(line == 0, names, jnp.where(line == 1, flags, 0.0)))
        ids = meta[STRETCH - HALO :, 0:1].astype(jnp.int32)
        items = table.shape[0]
        lane = lax.broadcasted_iota(jnp.int32, (HALO + events, items), 1)
        hot[u] = (ids == lane).astype(F32).astype(BF16)
        both = jnp.dot(hot[u], tin[:, heads * LANES :], preferred_element_type=F32)
        rowbuf[0] = both[:, :LANES]
        rowbuf[1] = both[:, LANES:]
        parts = jnp.dot(hot[u, pl.ds(HALO, events), :], tdt[...], preferred_element_type=F32)
        parts = jnp.transpose(parts)
        raw = parts[0:heads] + parts[heads : 2 * heads] + parts[2 * heads : 3 * heads]
        upper = jnp.where(line_rows <= line_cols, 1.0, 0.0).astype(F32)
        steps, paced = [], []
        for s in range(stretches):
            span = slice(s * STRETCH, (s + 1) * STRETCH)
            value = raw[:, span] + params[0]
            step = kept[:, span] * (jnp.maximum(value, 0.0) + jnp.log1p(jnp.exp(-jnp.abs(value))))
            steps.append(step)
            paced.append(step * params[1])
        sums = jnp.dot(
            jnp.concatenate(paced, axis=0),
            upper,
            precision=lax.Precision.HIGHEST,
            preferred_element_type=F32,
        )
        past = jnp.zeros((heads, LANES), F32)
        for s in range(stretches):
            log = sums[s * heads : (s + 1) * heads]
            step = steps[s]
            logs_t[u, s] = log
            steps_t[u, s] = step
            total = jnp.broadcast_to(log[:, STRETCH - 1 :], (heads, LANES))
            tail = jnp.exp(log - total) * step
            shrink = jnp.exp(-total)
            for p in range(heads):
                shrinks[u * per + p // rows, s, :, (p % rows) * LANES : (p % rows + 1) * LANES] = (
                    jnp.broadcast_to(shrink[p : p + 1], (8, LANES))
                )
            used = jnp.broadcast_to(kept[:, s * STRETCH : (s + 1) * STRETCH], (heads, LANES))
            facts[pl.ds(pl.multiple_of(u * events + s * STRETCH, STRETCH), STRETCH), :] = jnp.transpose(
                jnp.concatenate(
                    [log, tail, jnp.exp(-log), jnp.exp(-(log + past)), used]
                    + [jnp.zeros((LANES - 5 * heads, LANES), F32)],
                    axis=0,
                )
            )
            past = past + total
        for p in range(heads):
            aft[u, p % rows, p // rows] = jnp.broadcast_to(past[p : p + 1], (8, LANES))
        inward_t[u] = jnp.transpose(convolve(heads, 0)).astype(BF16)
        outward[pl.ds(pl.multiple_of(u * events, events), events), :] = convolve(heads + 1, 1).astype(BF16)
        for d in range(1, rows):
            log_copy(u, d).start()
        lin[u, r] = aft[u, r]

    def group(u, j):
        k = u * per + j
        mine = pl.ds(pl.multiple_of(u * events, events), events)
        gathered = jnp.dot(
            hot[u], tin[:, j * wide_group : (j + 1) * wide_group], preferred_element_type=F32
        )
        for q in range(rows):
            rowbuf[q] = gathered[:, q * LANES : (q + 1) * LANES]
        for q in range(rows):
            span = slice(q * LANES, (q + 1) * LANES)
            value = silu(convolve(j * rows + q, q)).astype(BF16)
            signal[u, j * rows + q] = value
            scaled[:, span] = (
                value.astype(F32)
                * facts[mine, heads + j * rows + q : heads + j * rows + q + 1]
            ).astype(BF16)
        run = None
        for s in range(stretches):
            span = slice(s * STRETCH, (s + 1) * STRETCH)
            added = jnp.dot(
                inward_t[u, :, span], scaled[span, :], preferred_element_type=F32
            )
            if run is None:
                held[k, s] = jnp.zeros_like(held[k, s])
                run = added
            else:
                held[k, s] = run.astype(BF16)
                run = run * shrinks[k, s, 0:1, :] + added
        for q in range(rows):
            ssend[k, q] = run[:, q * LANES : (q + 1) * LANES].astype(BF16)
        for d in range(1, rows):
            state_copy(k, d).start()

    def user_step(u, carry):
        prepare(u)
        for j in range(per):
            group(u, j)
        return carry

    lax.fori_loop(0, users, user_step, 0)

    def handle(k, carry):
        u, j = k // per, lax.rem(k, per)
        rin[k, r] = ssend[k, r]

        @pl.when(j == 0)
        def _():
            for d in range(1, rows):
                log_copy(u, d).wait_recv()

        for d in range(1, rows):
            state_copy(k, d).wait_recv()
        carried = jnp.zeros(pin.shape[1:], F32)
        fade = jnp.ones((1, LANES), F32)
        fades = []
        for m in range(rows):
            before[m] = carried
            fades.append(fade)
            here = jnp.exp(-lin[u, m, j, 0:1, :])
            carried = here * carried + rin[k, m].astype(F32)
            fade = fade * here

        @pl.when(c == 0)
        def _():
            pin[k] = jnp.zeros(pin.shape[1:], BF16)
            psend[k] = carried.astype(BF16)
            if cols > 1:
                onward_copy(k).start()

        if cols > 1:

            @pl.when(c > 0)
            def _():
                onward_copy(k).wait_recv()

            @pl.when(jnp.logical_and(c > 0, c < cols - 1))
            def _():
                psend[k] = (fade * pin[k].astype(F32) + carried).astype(BF16)
                onward_copy(k).start()

        for q in range(rows):
            esend[k, q] = (fades[q] * pin[k].astype(F32) + before[q]).astype(BF16)
        for d in range(1, rows):
            enter_copy(k, d).start()
        enter[k, r] = esend[k, r]
        return carry

    ticks = users * stretches

    def due(t):
        reach = (2 * t + 1 - 4 * c + 3 * 4 * cols) // 3 - 4 * cols + 1
        return jnp.minimum(jnp.maximum(reach, 0), pieces)

    chunk = inner // stretches

    def local_step(t, done):
        now = due(t)
        lax.fori_loop(done, now, handle, 0)
        u, s = t // stretches, lax.rem(t, stretches)
        span = pl.ds(pl.multiple_of(s * chunk, chunk), chunk)
        mine = pl.ds(pl.multiple_of(u * events, events), events)

        gates[mine, span] = silu(
            jnp.dot(hot[u, pl.ds(HALO, events), :], tgate[:, span], preferred_element_type=F32)
        )
        base = pl.multiple_of(s * STRETCH, STRETCH)
        place_rows = pl.ds(pl.multiple_of(u * events + s * STRETCH, STRETCH), STRETCH)
        seen = outward[place_rows, :]
        scores = jnp.dot(
            seen, inward_t[u, :, pl.ds(base, STRETCH)], preferred_element_type=F32
        )
        scores = jnp.where(causal, scores, 0.0)
        known = facts[place_rows, :]
        wide_seen = seen.astype(F32)
        for p in range(heads):
            h = head_of(p)
            gap = jnp.minimum(logs_t[u, s, p : p + 1, :] - known[:, p : p + 1], 0.0)
            weights = (jnp.exp(gap) * (scores * steps_t[u, s, p : p + 1, :])).astype(BF16)
            faded = (wide_seen * known[:, 2 * heads + p : 2 * heads + p + 1]).astype(BF16)
            q = p % rows
            right = jnp.concatenate(
                [
                    signal[u, p, pl.ds(base, STRETCH), :],
                    held[u * per + p // rows, s, :, q * LANES : (q + 1) * LANES],
                ],
                axis=0,
            )
            y[place_rows, h * LANES : (h + 1) * LANES] = jnp.dot(
                jnp.concatenate([weights, faded], axis=1), right, preferred_element_type=F32
            )
        return now

    done = lax.fori_loop(0, ticks, local_step, 0)
    lax.fori_loop(done, pieces, handle, 0)
    wout_copy.wait()

    def finish_step(u, carry):
        for j in range(per):
            for d in range(1, rows):
                enter_copy(u * per + j, d).wait_recv()
        for i in range(events // tall):
            span = pl.ds(pl.multiple_of(u * events + i * tall, tall), tall)
            squares = None
            for p in range(0, heads, 2):
                far = jnp.dot(
                    outward[span, :],
                    jnp.concatenate(
                        [enter[u * per + e // rows, e % rows] for e in (p, p + 1)], axis=1
                    ),
                    preferred_element_type=F32,
                )
                for e in (p, p + 1):
                    h = head_of(e)
                    where = slice(h * LANES, (h + 1) * LANES)
                    part = far[:, (e - p) * LANES : (e - p + 1) * LANES]
                    fade = facts[span, 3 * heads + e : 3 * heads + e + 1]
                    value = (y[span, where] + part * fade) * gates[span, where]
                    mix[i, :, where] = value
                    squares = value * value if squares is None else squares + value * value
            mean = jnp.sum(squares, axis=1, keepdims=True) * (1.0 / inner)
            normed = (mix[i] * lax.rsqrt(mean + 1.0) * gain_ref[...]).astype(BF16)
            result = jnp.dot(normed, wout[...], preferred_element_type=F32)
            out_ref[span, :] = (result * facts[span, 4 * heads : 4 * heads + 1]).astype(BF16)
        return carry

    lax.fori_loop(0, users, finish_step, 0)

    @pl.when(has_after)
    def _():
        halo_copy.wait_send()

    for u in range(users):
        for d in range(1, rows):
            log_copy(u, d).wait_send()
    for k in range(pieces):
        for d in range(1, rows):
            state_copy(k, d).wait_send()
            enter_copy(k, d).wait_send()
    if cols > 1:

        @pl.when(c < cols - 1)
        def _():
            for k in range(pieces):
                onward_copy(k).wait_send()


def per_device(
    item_ids,
    pad_masks,
    lengths,
    item_table,
    w_gate,
    w_in,
    w_dt,
    conv_taps,
    dt_bias,
    decay_rates,
    norm_gain,
    w_out,
):
    users, _, events = item_ids.shape
    items, model = item_table.shape
    full_width = w_in.shape[1]
    inner = w_gate.shape[1]
    heads = decay_rates.shape[0]
    state_width = (full_width - inner) // 2
    rows, cols = lax.axis_size("row"), lax.axis_size("col")
    stretches = events // STRETCH
    per = heads // rows
    pieces = users * per
    total = users * events
    tall = 2 * STRETCH if events % (2 * STRETCH) == 0 else STRETCH
    group = rows * LANES
    head = (state_width, LANES)

    vmem = pl.BlockSpec(memory_space=pltpu.VMEM)
    hbm = pl.BlockSpec(memory_space=pltpu.HBM)
    dma = pltpu.SemaphoreType.DMA

    def f32(*shape):
        return pltpu.VMEM(shape, F32)

    def bf16(*shape):
        return pltpu.VMEM(shape, BF16)

    result = pl.pallas_call(
        functools.partial(mixer_kernel, (rows, cols, users, heads, tall)),
        in_specs=[hbm] * 12,
        out_specs=vmem,
        out_shape=jax.ShapeDtypeStruct((total, w_out.shape[1]), BF16),
        scratch_shapes=[
            pltpu.SMEM(lengths.shape, jnp.int32),
            pltpu.VMEM(item_ids.shape, jnp.int32),
            pltpu.VMEM(pad_masks.shape, jnp.int32),
            bf16(*w_dt.shape[::-1]),
            f32(*conv_taps.shape),
            f32(1, heads),
            f32(1, heads),
            f32(1, inner),
            bf16(items, model),
            bf16(model, full_width),
            bf16(model, inner),
            bf16(*w_out.shape),
            bf16(items, full_width),
            bf16(items, inner),
            bf16(items, LANES),
            bf16(LANES, model),
            f32(2, heads, LANES),
            f32(heads + 2, 8, LANES),
            bf16(users, HALO + events, items),
            f32(max(rows, 2), HALO + events, LANES),
            bf16(users, state_width, events),
            bf16(total, state_width),
            f32(total, LANES),
            f32(users, stretches, heads, LANES),
            f32(users, stretches, heads, LANES),
            f32(pieces, stretches, 8, group),
            bf16(users, heads, events, LANES),
            bf16(events, group),
            bf16(pieces, stretches, state_width, group),
            bf16(pieces, rows, *head),
            bf16(pieces, rows, *head),
            f32(users, rows, per, 8, LANES),
            f32(users, rows, per, 8, LANES),
            f32(rows, *head),
            bf16(pieces, *head),
            bf16(pieces, *head),
            bf16(pieces, rows, *head),
            bf16(pieces, rows, *head),
            f32(total, inner),
            f32(total, inner),
            f32(events // tall, tall, inner),
            pltpu.VMEM((users, 1, STRETCH), jnp.int32),
            dma((heads + 5,)),
            dma((8,)),
            dma((2,)),
            dma((users, rows)),
            dma((users, rows)),
            dma((pieces, rows)),
            dma((pieces, rows)),
            dma((pieces,)),
            dma((pieces,)),
            dma((pieces, rows)),
            dma((pieces, rows)),
        ],
        compiler_params=pltpu.CompilerParams(
            collective_id=0, has_side_effects=True, vmem_limit_bytes=48 * 1024 * 1024
        ),
        name="mixer",
    )(
        *(
            pltpu.with_memory_space_constraint(array, pltpu.HBM)
            for array in (
                lengths,
                item_ids,
                pad_masks,
                w_dt.T,
                conv_taps,
                dt_bias[None],
                decay_rates[None],
                norm_gain[None],
                item_table,
                w_in,
                w_gate,
                w_out,
            )
        )
    )
    return result.reshape(users, 1, events, -1)


def solution(mesh):
    in_specs = (
        P("batch", "col", "row"),
        P("batch", "col", "row"),
        P("batch"),
        P(),
        P(),
        P(),
        P(),
        P(),
        P(),
        P(),
        P(),
        P(),
    )
    out_specs = P("batch", "col", "row", None)
    return jax.shard_map(
        per_device, mesh=mesh, in_specs=in_specs, out_specs=out_specs, check_vma=False
    )
```

```python
import functools

import jax
import jax.numpy as jnp
from jax import lax
from jax.experimental import pallas as pl
from jax.experimental.pallas import tpu as pltpu
from jax.sharding import PartitionSpec as P

STRETCH = 128
LANES = 128
HALO = 16
MESH = pl.DeviceIdType.MESH
F32 = jnp.float32
BF16 = jnp.bfloat16


def silu(v):
    return 0.5 * v * (1.0 + jnp.tanh(0.5 * v))


def remote(src, dst, send, recv, device):
    return pltpu.make_async_remote_copy(
        src_ref=src,
        dst_ref=dst,
        send_sem=send,
        recv_sem=recv,
        device_id=device,
        device_id_type=MESH,
    )


def mixer_kernel(
    counts,
    lengths_hbm,
    ids_hbm,
    masks_hbm,
    wdt_hbm,
    taps_hbm,
    bias_hbm,
    rates_hbm,
    gain_hbm,
    table_hbm,
    win_hbm,
    wgate_hbm,
    wout_hbm,
    out_ref,
    lengths_ref,
    ids_ref,
    masks_ref,
    wdt_ref,
    taps_ref,
    bias_ref,
    rates_ref,
    gain_ref,
    table,
    win,
    wgate,
    wout,
    tin,
    tgate,
    tdt,
    wide,
    params,
    ptaps,
    hot,
    rowbuf,
    inward_t,
    outward,
    facts,
    logs_t,
    steps_t,
    shrinks,
    signal,
    scaled,
    held,
    ssend,
    rin,
    aft,
    lin,
    before,
    fades,
    pin,
    nearin,
    farin,
    fadein,
    psend,
    fsend,
    esend,
    enter,
    y,
    gates,
    mix,
    sums,
    landed,
    wsem,
    psem,
    hsem,
    lsem_s,
    lsem_r,
    s1,
    r1,
    s2,
    r2,
    s3,
    r3,
    s4,
    r4,
    s5,
    r5,
):
    rows, cols, users, heads, tall = counts
    events = ids_ref.shape[2]
    stretches = events // STRETCH
    kernel = taps_ref.shape[0]
    inner = wgate.shape[1]
    per = heads // rows
    pieces = users * per
    wide_group = rows * LANES
    r, c = lax.axis_index("row"), lax.axis_index("col")
    place = c * rows + r
    places = rows * cols
    later = lax.rem(place + 1, places)
    earlier = lax.rem(place + places - 1, places)
    after = {"row": lax.rem(later, rows), "col": later // rows}
    ahead = {"row": lax.rem(earlier, rows), "col": earlier // rows}
    has_after, has_before = place < places - 1, place > 0
    wraps = jnp.logical_and(r == rows - 1, c < cols - 1)
    wrapped = jnp.logical_and(r == 0, c > 0)

    def head_of(p):
        return (p % rows) * per + p // rows

    def column(p):
        source = head_of(p) if not isinstance(p, int) or p < heads else p
        return pltpu.make_async_copy(
            win_hbm.at[:, pl.ds(source * LANES, LANES)],
            win.at[:, pl.ds(p * LANES, LANES)],
            wsem.at[p],
        )

    blocks = heads + 2
    table_copy = pltpu.make_async_copy(table_hbm, table, wsem.at[blocks])
    wgate_copy = pltpu.make_async_copy(wgate_hbm, wgate, wsem.at[blocks + 1])
    wout_copy = pltpu.make_async_copy(wout_hbm, wout, wsem.at[blocks + 2])
    small = [
        pltpu.make_async_copy(source, target, psem.at[i])
        for i, (source, target) in enumerate(
            (
                (ids_hbm, ids_ref),
                (masks_hbm, masks_ref),
                (lengths_hbm, lengths_ref),
                (wdt_hbm, wdt_ref),
                (taps_hbm, taps_ref),
                (bias_hbm, bias_ref),
                (rates_hbm, rates_ref),
                (gain_hbm, gain_ref),
            )
        )
    ]
    table_copy.start()
    for copy in small:
        copy.start()
    for p in (heads, heads + 1, *range(heads)):
        column(p).start()

    barrier = pltpu.get_barrier_semaphore()
    for d in range(1, rows):
        pl.semaphore_signal(
            barrier, inc=1, device_id={"row": lax.rem(r + d, rows)}, device_id_type=MESH
        )

    @pl.when(c > 0)
    def _():
        pl.semaphore_signal(barrier, inc=1, device_id={"col": c - 1}, device_id_type=MESH)

    @pl.when(c < cols - 1)
    def _():
        pl.semaphore_signal(barrier, inc=1, device_id={"col": c + 1}, device_id_type=MESH)

    @pl.when(c > 1)
    def _():
        pl.semaphore_signal(barrier, inc=1, device_id={"col": c - 2}, device_id_type=MESH)

    @pl.when(c < cols - 2)
    def _():
        pl.semaphore_signal(barrier, inc=1, device_id={"col": c + 2}, device_id_type=MESH)

    @pl.when(wraps)
    def _():
        pl.semaphore_signal(barrier, inc=1, device_id=after, device_id_type=MESH)

    @pl.when(wrapped)
    def _():
        pl.semaphore_signal(barrier, inc=1, device_id=ahead, device_id_type=MESH)

    halo_copy = remote(
        ids_ref.at[:, :, pl.ds(events - STRETCH, STRETCH)], landed, hsem.at[0], hsem.at[1], after
    )

    wide[...] = jnp.zeros_like(wide)
    for copy in small:
        copy.wait()
    line_rows = lax.broadcasted_iota(jnp.int32, (STRETCH, STRETCH), 0)
    line_cols = lax.broadcasted_iota(jnp.int32, (STRETCH, STRETCH), 1)
    causal = line_rows >= line_cols
    for i, source in enumerate((bias_ref, rates_ref)):
        value = jnp.zeros((heads, LANES), F32)
        for p in range(heads):
            value = jnp.where(line_rows[0:heads] == p, source[:, head_of(p) : head_of(p) + 1], value)
        params[i] = value
    wide[0:heads, :] = jnp.concatenate(
        [wdt_ref[head_of(p) : head_of(p) + 1, :] for p in range(heads)], axis=0
    )
    for p in range(blocks):
        source = p if p >= heads else head_of(p)
        ptaps[p, 0:kernel, :] = taps_ref[:, source * LANES : (source + 1) * LANES]

    table_copy.wait()

    def table_block(first):
        span = pl.ds(first, 2 * LANES)
        if not isinstance(first, int):
            span = pl.ds(pl.multiple_of(first, 2 * LANES), 2 * LANES)
        tin[:, span] = jnp.dot(table[...], win[:, span], preferred_element_type=F32).astype(BF16)

    column(heads).wait()
    column(heads + 1).wait()
    table_block(heads * LANES)

    raw = lax.dot_general(
        table[...], wide[...], (((1,), (1,)), ((), ())), preferred_element_type=F32
    )
    high = raw.astype(BF16).astype(F32)
    middle = (raw - high).astype(BF16).astype(F32)
    low = raw - high - middle
    tdt[...] = (high + pltpu.roll(middle, heads, 1) + pltpu.roll(low, 2 * heads, 1)).astype(BF16)

    peers = (
        rows
        - 1
        + jnp.where(c > 0, 1, 0)
        + jnp.where(c < cols - 1, 1, 0)
        + jnp.where(c > 1, 1, 0)
        + jnp.where(c < cols - 2, 1, 0)
        + jnp.where(wraps, 1, 0)
        + jnp.where(wrapped, 1, 0)
    )
    pl.semaphore_wait(barrier, peers)

    @pl.when(has_after)
    def _():
        halo_copy.start()

    def table_step(i, carry):
        column(2 * i).wait()
        column(2 * i + 1).wait()
        table_block(i * 2 * LANES)
        return carry

    lax.fori_loop(0, heads // 2, table_step, 0)
    wgate_copy.start()
    wout_copy.start()

    @pl.when(place == 0)
    def _():
        landed[...] = jnp.full(landed.shape, -1, jnp.int32)

    @pl.when(has_before)
    def _():
        halo_copy.wait_recv()

    def convolve(position, slot):
        total = None
        for k in range(kernel):
            part = rowbuf[slot, pl.ds(HALO - kernel + 1 + k, events), :] * ptaps[position, k : k + 1, :]
            total = part if total is None else total + part
        return total

    def log_copy(u, d):
        q = lax.rem(r + d, rows)
        return remote(
            aft.at[u, q], lin.at[u, r], lsem_s.at[u, d], lsem_r.at[u, d], {"row": q}
        )

    def state_copy(k, d):
        q = lax.rem(r + d, rows)
        return remote(ssend.at[k, q], rin.at[k, r], s1.at[k, d], r1.at[k, d], {"row": q})

    def near_copy(k):
        return remote(
            psend.at[k], nearin.at[k], s2.at[k], r2.at[k], {"col": lax.rem(c + 1, cols)}
        )

    def fade_copy(k):
        return remote(
            fsend.at[k], fadein.at[k], s4.at[k], r4.at[k], {"col": lax.rem(c + 1, cols)}
        )

    def far_copy(k):
        return remote(
            psend.at[k], farin.at[k], s5.at[k], r5.at[k], {"col": lax.rem(c + 2, cols)}
        )

    def enter_copy(k, d):
        q = lax.rem(r + d, rows)
        return remote(esend.at[k, q], enter.at[k, r], s3.at[k, d], r3.at[k, d], {"row": q})

    def prepare(u):
        first = place * events
        names = jnp.concatenate([landed[u], ids_ref[u]], axis=1).astype(F32)
        position = first + lax.broadcasted_iota(jnp.int32, (1, events), 1)
        kept = jnp.where(position < lengths_ref[u], masks_ref[u], 0)
        kept = jnp.where(kept > 0, 1.0, 0.0).astype(F32)
        flags = jnp.concatenate([jnp.zeros((1, STRETCH), F32), kept], axis=1)
        line = lax.broadcasted_iota(jnp.int32, (8, STRETCH + events), 0)
        meta = jnp.transpose(jnp.where(line == 0, names, jnp.where(line == 1, flags, 0.0)))
        ids = meta[STRETCH - HALO :, 0:1].astype(jnp.int32)
        items = table.shape[0]
        lane = lax.broadcasted_iota(jnp.int32, (HALO + events, items), 1)
        hot[u] = (ids == lane).astype(F32).astype(BF16)
        both = jnp.dot(hot[u], tin[:, heads * LANES :], preferred_element_type=F32)
        rowbuf[0] = both[:, :LANES]
        rowbuf[1] = both[:, LANES:]
        parts = jnp.dot(hot[u, pl.ds(HALO, events), :], tdt[...], preferred_element_type=F32)
        parts = jnp.transpose(parts)
        raw = parts[0:heads] + parts[heads : 2 * heads] + parts[2 * heads : 3 * heads]
        upper = jnp.where(line_rows <= line_cols, 1.0, 0.0).astype(F32)
        steps, paced = [], []
        for s in range(stretches):
            span = slice(s * STRETCH, (s + 1) * STRETCH)
            value = raw[:, span] + params[0]
            step = kept[:, span] * (jnp.maximum(value, 0.0) + jnp.log1p(jnp.exp(-jnp.abs(value))))
            steps.append(step)
            paced.append(step * params[1])
        sums = jnp.dot(
            jnp.concatenate(paced, axis=0),
            upper,
            precision=lax.Precision.HIGHEST,
            preferred_element_type=F32,
        )
        past = jnp.zeros((heads, LANES), F32)
        for s in range(stretches):
            log = sums[s * heads : (s + 1) * heads]
            step = steps[s]
            logs_t[u, s] = log
            steps_t[u, s] = step
            total = jnp.broadcast_to(log[:, STRETCH - 1 :], (heads, LANES))
            tail = jnp.exp(log - total) * step
            shrink = jnp.exp(-total)
            for p in range(heads):
                shrinks[u * per + p // rows, s, :, (p % rows) * LANES : (p % rows + 1) * LANES] = (
                    jnp.broadcast_to(shrink[p : p + 1], (8, LANES))
                )
            used = jnp.broadcast_to(kept[:, s * STRETCH : (s + 1) * STRETCH], (heads, LANES))
            facts[pl.ds(pl.multiple_of(u * events + s * STRETCH, STRETCH), STRETCH), :] = jnp.transpose(
                jnp.concatenate(
                    [log, tail, jnp.exp(-log), jnp.exp(-(log + past)), used]
                    + [jnp.zeros((LANES - 5 * heads, LANES), F32)],
                    axis=0,
                )
            )
            past = past + total
        for p in range(heads):
            aft[u, p % rows, p // rows] = jnp.broadcast_to(past[p : p + 1], (8, LANES))
        inward_t[u] = jnp.transpose(convolve(heads, 0)).astype(BF16)
        outward[pl.ds(pl.multiple_of(u * events, events), events), :] = convolve(heads + 1, 1).astype(BF16)
        for d in range(1, rows):
            log_copy(u, d).start()
        lin[u, r] = aft[u, r]

    def group(u, j):
        k = u * per + j
        mine = pl.ds(pl.multiple_of(u * events, events), events)
        gathered = jnp.dot(
            hot[u], tin[:, j * wide_group : (j + 1) * wide_group], preferred_element_type=F32
        )
        for q in range(rows):
            rowbuf[q] = gathered[:, q * LANES : (q + 1) * LANES]
        for q in range(rows):
            span = slice(q * LANES, (q + 1) * LANES)
            value = silu(convolve(j * rows + q, q)).astype(BF16)
            signal[u, j * rows + q] = value
            scaled[:, span] = (
                value.astype(F32)
                * facts[mine, heads + j * rows + q : heads + j * rows + q + 1]
            ).astype(BF16)
        run = None
        for s in range(stretches):
            span = slice(s * STRETCH, (s + 1) * STRETCH)
            added = jnp.dot(
                inward_t[u, :, span], scaled[span, :], preferred_element_type=F32
            )
            if run is None:
                held[k, s] = jnp.zeros_like(held[k, s])
                run = added
            else:
                held[k, s] = run.astype(BF16)
                run = run * shrinks[k, s, 0:1, :] + added
        for q in range(rows):
            ssend[k, q] = run[:, q * LANES : (q + 1) * LANES].astype(BF16)
        for d in range(1, rows):
            state_copy(k, d).start()

    def user_step(u, carry):
        prepare(u)
        for j in range(per):
            group(u, j)
        return carry

    lax.fori_loop(0, users, user_step, 0)

    odd = lax.rem(c, 2) == 1
    gives_own = jnp.logical_and(jnp.logical_not(odd), c < cols - 1)
    gives_near = jnp.logical_and(odd, c < cols - 1)
    gives_far = jnp.logical_and(odd, c < cols - 2)
    takes_far = jnp.logical_and(odd, c > 1)

    def gather_piece(k, carry):
        u, j = k // per, lax.rem(k, per)
        rin[k, r] = ssend[k, r]

        @pl.when(j == 0)
        def _():
            for d in range(1, rows):
                log_copy(u, d).wait_recv()

        for d in range(1, rows):
            state_copy(k, d).wait_recv()
        carried = jnp.zeros(nearin.shape[1:], F32)
        fade = jnp.ones((8, LANES), F32)
        for m in range(rows):
            before[k, m] = carried
            fades[k, m] = fade
            here = jnp.exp(-lin[u, m, j])
            carried = here[0:1] * carried + rin[k, m].astype(F32)
            fade = fade * here
        before[k, rows] = carried
        fades[k, rows] = fade
        if cols > 1:

            @pl.when(gives_own)
            def _():
                psend[k] = carried.astype(BF16)
                fsend[k] = fade
                near_copy(k).start()
                fade_copy(k).start()

        return carry

    def enter_piece(k, carry):
        @pl.when(c == 0)
        def _():
            pin[...] = jnp.zeros_like(pin)

        if cols > 1:

            @pl.when(c > 0)
            def _():
                near_copy(k).wait_recv()
                pin[...] = nearin[k].astype(F32)

            @pl.when(odd)
            def _():
                fade_copy(k).wait_recv()

            @pl.when(takes_far)
            def _():
                far_copy(k).wait_recv()
                pin[...] = fadein[k, 0:1] * farin[k].astype(F32) + nearin[k].astype(F32)

            @pl.when(gives_near)
            def _():
                psend[k] = (fades[k, rows, 0:1] * pin[...] + before[k, rows]).astype(BF16)
                near_copy(k).start()

            @pl.when(gives_far)
            def _():
                far_copy(k).start()

        for q in range(rows):
            esend[k, q] = (fades[k, q, 0:1] * pin[...] + before[k, q]).astype(BF16)
        for d in range(1, rows):
            enter_copy(k, d).start()
        enter[k, r] = esend[k, r]
        return carry

    ticks = users * stretches

    def due(t):
        return jnp.minimum(jnp.maximum(t, 0) // 2, pieces)

    lag = jnp.where(c == 0, 0, 4 * ((c + 2) // 2))

    wgate_copy.wait()
    chunk = inner // stretches

    def local_step(t, done):
        now = due(t + 1), due(t + 1 - lag)
        lax.fori_loop(done[0], now[0], gather_piece, 0)
        lax.fori_loop(done[1], now[1], enter_piece, 0)
        u, s = t // stretches, lax.rem(t, stretches)
        span = pl.ds(pl.multiple_of(s * chunk, chunk), chunk)
        mine = pl.ds(pl.multiple_of(u * events, events), events)

        @pl.when(u == 0)
        def _():
            tgate[:, span] = jnp.dot(
                table[...], wgate[:, span], preferred_element_type=F32
            ).astype(BF16)

        gates[mine, span] = silu(
            jnp.dot(hot[u, pl.ds(HALO, events), :], tgate[:, span], preferred_element_type=F32)
        )
        base = pl.multiple_of(s * STRETCH, STRETCH)
        place_rows = pl.ds(pl.multiple_of(u * events + s * STRETCH, STRETCH), STRETCH)
        seen = outward[place_rows, :]
        scores = jnp.dot(
            seen, inward_t[u, :, pl.ds(base, STRETCH)], preferred_element_type=F32
        )
        scores = jnp.where(causal, scores, 0.0)
        known = facts[place_rows, :]
        wide_seen = seen.astype(F32)
        for p in range(heads):
            h = head_of(p)
            gap = jnp.minimum(logs_t[u, s, p : p + 1, :] - known[:, p : p + 1], 0.0)
            weights = (jnp.exp(gap) * (scores * steps_t[u, s, p : p + 1, :])).astype(BF16)
            faded = (wide_seen * known[:, 2 * heads + p : 2 * heads + p + 1]).astype(BF16)
            q = p % rows
            right = jnp.concatenate(
                [
                    signal[u, p, pl.ds(base, STRETCH), :],
                    held[u * per + p // rows, s, :, q * LANES : (q + 1) * LANES],
                ],
                axis=0,
            )
            y[place_rows, h * LANES : (h + 1) * LANES] = jnp.dot(
                jnp.concatenate([weights, faded], axis=1), right, preferred_element_type=F32
            )
        return now

    done = lax.fori_loop(0, ticks, local_step, (0, 0))
    lax.fori_loop(done[0], pieces, gather_piece, 0)
    lax.fori_loop(done[1], pieces, enter_piece, 0)
    wout_copy.wait()

    def finish_step(u, carry):
        def rows_of(i):
            return pl.ds(pl.multiple_of(u * events + i * tall, tall), tall)

        for j in range(per):
            for d in range(1, rows):
                enter_copy(u * per + j, d).wait_recv()
            for i in range(events // tall):
                span = rows_of(i)
                squares = None
                for q in range(0, rows, 2):
                    pair = range(q, min(q + 2, rows))
                    far = jnp.dot(
                        outward[span, :],
                        jnp.concatenate([enter[u * per + j, e] for e in pair], axis=1),
                        preferred_element_type=F32,
                    )
                    for e in pair:
                        h = e * per + j
                        p = j * rows + e
                        where = slice(h * LANES, (h + 1) * LANES)
                        part = far[:, (e - q) * LANES : (e - q + 1) * LANES]
                        fade = facts[span, 3 * heads + p : 3 * heads + p + 1]
                        value = (y[span, where] + part * fade) * gates[span, where]
                        mix[i, :, where] = value
                        squares = value * value if squares is None else squares + value * value
                if j == 0:
                    sums[i] = squares
                else:
                    sums[i] += squares
        for i in range(events // tall):
            span = rows_of(i)
            mean = jnp.sum(sums[i], axis=1, keepdims=True) * (1.0 / inner)
            normed = (mix[i] * lax.rsqrt(mean + 1.0) * gain_ref[...]).astype(BF16)
            result = jnp.dot(normed, wout[...], preferred_element_type=F32)
            out_ref[span, :] = (result * facts[span, 4 * heads : 4 * heads + 1]).astype(BF16)
        return carry

    lax.fori_loop(0, users, finish_step, 0)

    @pl.when(has_after)
    def _():
        halo_copy.wait_send()

    for u in range(users):
        for d in range(1, rows):
            log_copy(u, d).wait_send()
    for k in range(pieces):
        for d in range(1, rows):
            state_copy(k, d).wait_send()
            enter_copy(k, d).wait_send()
    if cols > 1:

        @pl.when(c < cols - 1)
        def _():
            for k in range(pieces):
                near_copy(k).wait_send()

        @pl.when(gives_own)
        def _():
            for k in range(pieces):
                fade_copy(k).wait_send()

        @pl.when(gives_far)
        def _():
            for k in range(pieces):
                far_copy(k).wait_send()


def per_device(
    item_ids,
    pad_masks,
    lengths,
    item_table,
    w_gate,
    w_in,
    w_dt,
    conv_taps,
    dt_bias,
    decay_rates,
    norm_gain,
    w_out,
):
    users, _, events = item_ids.shape
    items, model = item_table.shape
    full_width = w_in.shape[1]
    inner = w_gate.shape[1]
    heads = decay_rates.shape[0]
    state_width = (full_width - inner) // 2
    rows, cols = lax.axis_size("row"), lax.axis_size("col")
    stretches = events // STRETCH
    per = heads // rows
    pieces = users * per
    total = users * events
    tall = 2 * STRETCH if events % (2 * STRETCH) == 0 else STRETCH
    group = rows * LANES
    head = (state_width, LANES)

    vmem = pl.BlockSpec(memory_space=pltpu.VMEM)
    hbm = pl.BlockSpec(memory_space=pltpu.HBM)
    dma = pltpu.SemaphoreType.DMA

    def f32(*shape):
        return pltpu.VMEM(shape, F32)

    def bf16(*shape):
        return pltpu.VMEM(shape, BF16)

    result = pl.pallas_call(
        functools.partial(mixer_kernel, (rows, cols, users, heads, tall)),
        in_specs=[hbm] * 12,
        out_specs=vmem,
        out_shape=jax.ShapeDtypeStruct((total, w_out.shape[1]), BF16),
        scratch_shapes=[
            pltpu.SMEM(lengths.shape, jnp.int32),
            pltpu.VMEM(item_ids.shape, jnp.int32),
            pltpu.VMEM(pad_masks.shape, jnp.int32),
            bf16(*w_dt.shape[::-1]),
            f32(*conv_taps.shape),
            f32(1, heads),
            f32(1, heads),
            f32(1, inner),
            bf16(items, model),
            bf16(model, full_width),
            bf16(model, inner),
            bf16(*w_out.shape),
            bf16(items, full_width),
            bf16(items, inner),
            bf16(items, LANES),
            bf16(LANES, model),
            f32(2, heads, LANES),
            f32(heads + 2, 8, LANES),
            bf16(users, HALO + events, items),
            f32(max(rows, 2), HALO + events, LANES),
            bf16(users, state_width, events),
            bf16(total, state_width),
            f32(total, LANES),
            f32(users, stretches, heads, LANES),
            f32(users, stretches, heads, LANES),
            f32(pieces, stretches, 8, group),
            bf16(users, heads, events, LANES),
            bf16(events, group),
            bf16(pieces, stretches, state_width, group),
            bf16(pieces, rows, *head),
            bf16(pieces, rows, *head),
            f32(users, rows, per, 8, LANES),
            f32(users, rows, per, 8, LANES),
            f32(pieces, rows + 1, *head),
            f32(pieces, rows + 1, 8, LANES),
            f32(*head),
            bf16(pieces, *head),
            bf16(pieces, *head),
            f32(pieces, 8, LANES),
            bf16(pieces, *head),
            f32(pieces, 8, LANES),
            bf16(pieces, rows, *head),
            bf16(pieces, rows, *head),
            f32(total, inner),
            f32(total, inner),
            f32(events // tall, tall, inner),
            f32(events // tall, tall, LANES),
            pltpu.VMEM((users, 1, STRETCH), jnp.int32),
            dma((heads + 5,)),
            dma((8,)),
            dma((2,)),
            dma((users, rows)),
            dma((users, rows)),
            dma((pieces, rows)),
            dma((pieces, rows)),
            dma((pieces,)),
            dma((pieces,)),
            dma((pieces, rows)),
            dma((pieces, rows)),
            dma((pieces,)),
            dma((pieces,)),
            dma((pieces,)),
            dma((pieces,)),
        ],
        compiler_params=pltpu.CompilerParams(
            collective_id=0, has_side_effects=True, vmem_limit_bytes=48 * 1024 * 1024
        ),
        name="mixer",
    )(
        *(
            pltpu.with_memory_space_constraint(array, pltpu.HBM)
            for array in (
                lengths,
                item_ids,
                pad_masks,
                w_dt.T,
                conv_taps,
                dt_bias[None],
                decay_rates[None],
                norm_gain[None],
                item_table,
                w_in,
                w_gate,
                w_out,
            )
        )
    )
    return result.reshape(users, 1, events, -1)


def solution(mesh):
    in_specs = (
        P("batch", "col", "row"),
        P("batch", "col", "row"),
        P("batch"),
        P(),
        P(),
        P(),
        P(),
        P(),
        P(),
        P(),
        P(),
        P(),
    )
    out_specs = P("batch", "col", "row", None)
    return jax.shard_map(
        per_device, mesh=mesh, in_specs=in_specs, out_specs=out_specs, check_vma=False
    )
```

```python
import functools

import jax
import jax.numpy as jnp
from jax import lax
from jax.experimental import pallas as pl
from jax.experimental.pallas import tpu as pltpu
from jax.sharding import PartitionSpec as P

STRETCH = 128
LANES = 128
HALO = 16
MESH = pl.DeviceIdType.MESH
F32 = jnp.float32
BF16 = jnp.bfloat16


def silu_of_twice(half):
    return half * (1.0 + jnp.tanh(half))


def remote(src, dst, send, recv, device):
    return pltpu.make_async_remote_copy(
        src_ref=src,
        dst_ref=dst,
        send_sem=send,
        recv_sem=recv,
        device_id=device,
        device_id_type=MESH,
    )


def mixer_kernel(
    counts,
    lengths_hbm,
    ids_hbm,
    masks_hbm,
    wdt_hbm,
    taps_hbm,
    bias_hbm,
    rates_hbm,
    gain_hbm,
    table_hbm,
    win_hbm,
    wgate_hbm,
    wout_hbm,
    out_ref,
    lengths_ref,
    ids_ref,
    masks_ref,
    wdt_ref,
    taps_ref,
    bias_ref,
    rates_ref,
    gain_ref,
    table,
    win,
    wgate,
    wout,
    tin,
    tgate,
    tdt,
    wide,
    params,
    ptaps,
    hot,
    rowbuf,
    inward_t,
    outward,
    facts,
    logs_t,
    steps_t,
    shrinks,
    signal,
    scaled,
    held,
    ssend,
    rin,
    aft,
    lin,
    before,
    fades,
    pin,
    nearin,
    farin,
    fadein,
    psend,
    fsend,
    esend,
    enter,
    y,
    gates,
    mix,
    sums,
    partial,
    landed,
    wsem,
    psem,
    hsem,
    lsem_s,
    lsem_r,
    s1,
    r1,
    s2,
    r2,
    s3,
    r3,
    s4,
    r4,
    s5,
    r5,
):
    rows, cols, users, heads, tall, parts = counts
    events = ids_ref.shape[2]
    stretches = events // STRETCH
    kernel = taps_ref.shape[0]
    inner = wgate.shape[1]
    per = heads // rows
    pieces = users * per * parts
    piece_rows = nearin.shape[1]
    wide_group = rows * LANES
    r, c = lax.axis_index("row"), lax.axis_index("col")
    place = c * rows + r
    places = rows * cols
    later = lax.rem(place + 1, places)
    earlier = lax.rem(place + places - 1, places)
    after = {"row": lax.rem(later, rows), "col": later // rows}
    ahead = {"row": lax.rem(earlier, rows), "col": earlier // rows}
    has_after, has_before = place < places - 1, place > 0
    wraps = jnp.logical_and(r == rows - 1, c < cols - 1)
    wrapped = jnp.logical_and(r == 0, c > 0)

    def head_of(p):
        return (p % rows) * per + p // rows

    win_parts = 4
    win_rows = win.shape[0] // win_parts

    def win_copy(i):
        lines = pl.ds(i * win_rows, win_rows)
        return pltpu.make_async_copy(win_hbm.at[lines, :], win.at[lines, :], wsem.at[i])

    blocks = heads + 2
    table_copy = pltpu.make_async_copy(table_hbm, table, wsem.at[blocks])
    wgate_copy = pltpu.make_async_copy(wgate_hbm, wgate, wsem.at[blocks + 1])

    def wout_copy(p):
        return pltpu.make_async_copy(
            wout_hbm.at[pl.ds(head_of(p) * LANES, LANES), :],
            wout.at[pl.ds(p * LANES, LANES), :],
            wsem.at[blocks + 2 + p],
        )
    small = [
        pltpu.make_async_copy(source, target, psem.at[i])
        for i, (source, target) in enumerate(
            (
                (ids_hbm, ids_ref),
                (masks_hbm, masks_ref),
                (lengths_hbm, lengths_ref),
                (wdt_hbm, wdt_ref),
                (taps_hbm, taps_ref),
                (bias_hbm, bias_ref),
                (rates_hbm, rates_ref),
                (gain_hbm, gain_ref),
            )
        )
    ]
    for copy in small:
        copy.start()
    table_copy.start()
    for i in range(win_parts):
        win_copy(i).start()

    barrier = pltpu.get_barrier_semaphore()
    for d in range(1, rows):
        pl.semaphore_signal(
            barrier, inc=1, device_id={"row": lax.rem(r + d, rows)}, device_id_type=MESH
        )

    @pl.when(c > 0)
    def _():
        pl.semaphore_signal(barrier, inc=1, device_id={"col": c - 1}, device_id_type=MESH)

    @pl.when(c < cols - 1)
    def _():
        pl.semaphore_signal(barrier, inc=1, device_id={"col": c + 1}, device_id_type=MESH)

    @pl.when(c > 1)
    def _():
        pl.semaphore_signal(barrier, inc=1, device_id={"col": c - 2}, device_id_type=MESH)

    @pl.when(c < cols - 2)
    def _():
        pl.semaphore_signal(barrier, inc=1, device_id={"col": c + 2}, device_id_type=MESH)

    @pl.when(wraps)
    def _():
        pl.semaphore_signal(barrier, inc=1, device_id=after, device_id_type=MESH)

    @pl.when(wrapped)
    def _():
        pl.semaphore_signal(barrier, inc=1, device_id=ahead, device_id_type=MESH)

    halo_copy = remote(
        ids_ref.at[:, :, pl.ds(events - STRETCH, STRETCH)], landed, hsem.at[0], hsem.at[1], after
    )

    wide[...] = jnp.zeros_like(wide)
    for copy in small:
        copy.wait()
    peers = (
        rows
        - 1
        + jnp.where(c > 0, 1, 0)
        + jnp.where(c < cols - 1, 1, 0)
        + jnp.where(c > 1, 1, 0)
        + jnp.where(c < cols - 2, 1, 0)
        + jnp.where(wraps, 1, 0)
        + jnp.where(wrapped, 1, 0)
    )
    pl.semaphore_wait(barrier, peers)

    @pl.when(has_after)
    def _():
        halo_copy.start()

    line_rows = lax.broadcasted_iota(jnp.int32, (STRETCH, STRETCH), 0)
    line_cols = lax.broadcasted_iota(jnp.int32, (STRETCH, STRETCH), 1)
    causal = line_rows >= line_cols
    for i, source in enumerate((bias_ref, rates_ref)):
        value = jnp.zeros((heads, LANES), F32)
        for p in range(heads):
            value = jnp.where(line_rows[0:heads] == p, source[:, head_of(p) : head_of(p) + 1], value)
        params[i] = value
    wide[0:heads, :] = jnp.concatenate(
        [wdt_ref[head_of(p) : head_of(p) + 1, :] for p in range(heads)], axis=0
    )
    for p in range(blocks):
        source = p if p >= heads else head_of(p)
        scale = 0.5 if p < heads else 1.0
        ptaps[p, 0:kernel, :] = scale * taps_ref[:, source * LANES : (source + 1) * LANES]

    table_copy.wait()

    for i in range(win_parts):
        win_copy(i).wait()

    def table_pair(first, left, right):
        weights = jnp.concatenate([win[:, left], win[:, right]], axis=1)
        tin[:, pl.ds(first, 2 * LANES)] = jnp.dot(
            table[...], weights, preferred_element_type=F32
        ).astype(BF16)

    table_pair(
        heads * LANES,
        slice(heads * LANES, (heads + 1) * LANES),
        slice((heads + 1) * LANES, (heads + 2) * LANES),
    )

    raw = lax.dot_general(
        wide[...], table[...], (((1,), (1,)), ((), ())), preferred_element_type=F32
    )[0:heads]
    high = raw.astype(BF16).astype(F32)
    middle = (raw - high).astype(BF16).astype(F32)
    low = raw - high - middle
    tdt[...] = jnp.concatenate([high, middle, low, jnp.zeros_like(low)], axis=0).astype(BF16)

    def table_step(i, carry):
        left, right = (
            pl.ds(pl.multiple_of(head_of(2 * i + e) * LANES, LANES), LANES) for e in (0, 1)
        )
        table_pair(pl.multiple_of(i * 2 * LANES, 2 * LANES), left, right)
        return carry

    lax.fori_loop(0, heads // 2, table_step, 0)
    wgate_copy.start()
    for p in range(heads):
        wout_copy(p).start()

    @pl.when(place == 0)
    def _():
        landed[...] = jnp.full(landed.shape, -1, jnp.int32)

    @pl.when(has_before)
    def _():
        halo_copy.wait_recv()

    def convolve(position):
        total = None
        for k in range(kernel):
            part = rowbuf[position, pl.ds(HALO - kernel + 1 + k, events), :] * ptaps[position, k : k + 1, :]
            total = part if total is None else total + part
        return total

    def log_copy(u, d):
        q = lax.rem(r + d, rows)
        return remote(
            aft.at[u, q], lin.at[u, r], lsem_s.at[u, d], lsem_r.at[u, d], {"row": q}
        )

    def state_copy(k, d):
        q = lax.rem(r + d, rows)
        return remote(ssend.at[k, q], rin.at[k, r], s1.at[k, d], r1.at[k, d], {"row": q})

    def near_copy(k):
        return remote(
            psend.at[k], nearin.at[k], s2.at[k], r2.at[k], {"col": lax.rem(c + 1, cols)}
        )

    def fade_copy(k):
        return remote(
            fsend.at[k], fadein.at[k], s4.at[k], r4.at[k], {"col": lax.rem(c + 1, cols)}
        )

    def far_copy(k):
        return remote(
            psend.at[k], farin.at[k], s5.at[k], r5.at[k], {"col": lax.rem(c + 2, cols)}
        )

    def enter_copy(k, d):
        q = lax.rem(r + d, rows)
        return remote(esend.at[k, q], enter.at[k, r], s3.at[k, d], r3.at[k, d], {"row": q})

    def prepare(u):
        first = place * events
        names = jnp.concatenate([landed[u], ids_ref[u]], axis=1).astype(F32)
        position = first + lax.broadcasted_iota(jnp.int32, (1, events), 1)
        kept = jnp.where(position < lengths_ref[u], masks_ref[u], 0)
        kept = jnp.where(kept > 0, 1.0, 0.0).astype(F32)
        flags = jnp.concatenate([jnp.zeros((1, STRETCH), F32), kept], axis=1)
        line = lax.broadcasted_iota(jnp.int32, (8, STRETCH + events), 0)
        meta = jnp.transpose(jnp.where(line == 0, names, jnp.where(line == 1, flags, 0.0)))
        ids = meta[STRETCH - HALO :, 0:1].astype(jnp.int32)
        items = table.shape[0]
        lane = lax.broadcasted_iota(jnp.int32, (HALO + events, items), 1)
        hot[u] = (ids == lane).astype(F32).astype(BF16)
        shares = lax.dot_general(
            tdt[...],
            hot[u, pl.ds(HALO, events), :],
            (((1,), (1,)), ((), ())),
            preferred_element_type=F32,
        )
        gather_pair(u, heads // 2)
        gather_pair(u, 0)
        raw = shares[0:heads] + shares[heads : 2 * heads] + shares[2 * heads : 3 * heads]
        upper = jnp.where(line_rows <= line_cols, 1.0, 0.0).astype(F32)
        steps, paced = [], []
        for s in range(stretches):
            span = slice(s * STRETCH, (s + 1) * STRETCH)
            value = raw[:, span] + params[0]
            step = kept[:, span] * (jnp.maximum(value, 0.0) + jnp.log1p(jnp.exp(-jnp.abs(value))))
            steps.append(step)
            paced.append(step * params[1])
        sums = jnp.dot(
            jnp.concatenate(paced, axis=0),
            upper,
            precision=lax.Precision.HIGHEST,
            preferred_element_type=F32,
        )
        past = jnp.zeros((heads, LANES), F32)
        for s in range(stretches):
            log = sums[s * heads : (s + 1) * heads]
            step = steps[s]
            logs_t[u, s] = log
            steps_t[u, s] = step
            total = jnp.broadcast_to(log[:, STRETCH - 1 :], (heads, LANES))
            tail = jnp.exp(log - total) * step
            shrink = jnp.exp(-total)
            for p in range(heads):
                shrinks[u * per + p // rows, s, :, (p % rows) * LANES : (p % rows + 1) * LANES] = (
                    jnp.broadcast_to(shrink[p : p + 1], (8, LANES))
                )
            used = jnp.broadcast_to(kept[:, s * STRETCH : (s + 1) * STRETCH], (heads, LANES))
            facts[pl.ds(pl.multiple_of(u * events + s * STRETCH, STRETCH), STRETCH), :] = jnp.transpose(
                jnp.concatenate(
                    [log, tail, jnp.exp(-log), jnp.exp(-(log + past)), used]
                    + [jnp.zeros((LANES - 5 * heads, LANES), F32)],
                    axis=0,
                )
            )
            past = past + total
        for p in range(heads):
            aft[u, p % rows, p // rows] = jnp.broadcast_to(past[p : p + 1], (8, LANES))
        inward_t[u] = jnp.transpose(convolve(heads)).astype(BF16)
        outward[pl.ds(pl.multiple_of(u * events, events), events), :] = convolve(heads + 1).astype(BF16)
        for d in range(1, rows):
            log_copy(u, d).start()
        lin[u, r] = aft[u, r]

    def gather_pair(u, a):
        both = jnp.dot(
            hot[u], tin[:, 2 * a * LANES : 2 * (a + 1) * LANES], preferred_element_type=F32
        )
        rowbuf[2 * a] = both[:, :LANES]
        rowbuf[2 * a + 1] = both[:, LANES:]

    def convert(u, p):
        mine = pl.ds(pl.multiple_of(u * events, events), events)
        j, q = p // rows, p % rows
        value = silu_of_twice(convolve(p)).astype(BF16)
        signal[u, p] = value
        scaled[j, :, q * LANES : (q + 1) * LANES] = (
            value.astype(F32) * facts[mine, heads + p : heads + p + 1]
        ).astype(BF16)

    def form_state(u, j):
        k = u * per + j
        run = None
        for s in range(stretches):
            span = slice(s * STRETCH, (s + 1) * STRETCH)
            added = jnp.dot(
                inward_t[u, :, span], scaled[j, span, :], preferred_element_type=F32
            )
            if run is None:
                held[k, s] = jnp.zeros_like(held[k, s])
                run = added
            else:
                held[k, s] = run.astype(BF16)
                run = run * shrinks[k, s, 0:1, :] + added
        for i in range(parts):
            lines = slice(i * piece_rows, (i + 1) * piece_rows)
            for q in range(rows):
                ssend[k * parts + i, q] = run[lines, q * LANES : (q + 1) * LANES].astype(BF16)
            for d in range(1, rows):
                state_copy(k * parts + i, d).start()

    def user_step(u, carry):
        prepare(u)
        for a in range(heads // 2):
            if a + 1 < heads // 2:
                gather_pair(u, a + 1)
            convert(u, 2 * a)
            convert(u, 2 * a + 1)
            for j in range(per):
                if 2 * a < (j + 1) * rows <= 2 * a + 2:
                    form_state(u, j)
        return carry

    lax.fori_loop(0, users, user_step, 0)

    odd = lax.rem(c, 2) == 1
    gives_own = jnp.logical_and(jnp.logical_not(odd), c < cols - 1)
    gives_near = jnp.logical_and(odd, c < cols - 1)
    gives_far = jnp.logical_and(odd, c < cols - 2)
    takes_far = jnp.logical_and(odd, c > 1)

    def gather_piece(k, carry):
        u, j = k // (per * parts), lax.rem(k // parts, per)
        rin[k, r] = ssend[k, r]

        @pl.when(lax.rem(k, per * parts) == 0)
        def _():
            for d in range(1, rows):
                log_copy(u, d).wait_recv()

        for d in range(1, rows):
            state_copy(k, d).wait_recv()
        carried = jnp.zeros(nearin.shape[1:], F32)
        fade = jnp.ones((8, LANES), F32)
        for m in range(rows):
            before[k, m] = carried
            fades[k, m] = fade
            here = jnp.exp(-lin[u, m, j])
            carried = here[0:1] * carried + rin[k, m].astype(F32)
            fade = fade * here
        before[k, rows] = carried
        fades[k, rows] = fade
        if cols > 1:

            @pl.when(gives_own)
            def _():
                psend[k] = carried.astype(BF16)
                fsend[k] = fade
                near_copy(k).start()
                fade_copy(k).start()

        return carry

    def enter_piece(k, carry):
        @pl.when(c == 0)
        def _():
            pin[...] = jnp.zeros_like(pin)

        if cols > 1:

            @pl.when(c > 0)
            def _():
                near_copy(k).wait_recv()
                pin[...] = nearin[k].astype(F32)

            @pl.when(odd)
            def _():
                fade_copy(k).wait_recv()

            @pl.when(takes_far)
            def _():
                far_copy(k).wait_recv()
                pin[...] = fadein[k, 0:1] * farin[k].astype(F32) + nearin[k].astype(F32)

            @pl.when(gives_near)
            def _():
                psend[k] = (fades[k, rows, 0:1] * pin[...] + before[k, rows]).astype(BF16)

            @pl.when(gives_far)
            def _():
                far_copy(k).start()

            @pl.when(gives_near)
            def _():
                near_copy(k).start()

        for q in range(rows):
            esend[k, q] = (fades[k, q, 0:1] * pin[...] + before[k, q]).astype(BF16)
        for d in range(1, rows):
            enter_copy(k, d).start()
        enter[k, r] = esend[k, r]
        return carry

    ticks = users * stretches

    def due(t):
        t = jnp.maximum(t, -1) + stretches
        whole, rest = t // stretches - 1, lax.rem(t, stretches)
        return jnp.minimum(jnp.maximum(whole * per + jnp.minimum(rest + 1, per), 0) * parts, pieces)

    lag = jnp.where(c == 0, 0, 4 * ((c + 2) // 2))

    wgate_copy.wait()
    chunk = inner // stretches

    def local_step(t, done):
        now = due(t), due(t - lag)
        lax.fori_loop(done[0], now[0], gather_piece, 0)
        lax.fori_loop(done[1], now[1], enter_piece, 0)
        u, s = t // stretches, lax.rem(t, stretches)
        span = pl.ds(pl.multiple_of(s * chunk, chunk), chunk)
        mine = pl.ds(pl.multiple_of(u * events, events), events)

        @pl.when(u == 0)
        def _():
            tgate[:, span] = (
                0.5 * jnp.dot(table[...], wgate[:, span], preferred_element_type=F32)
            ).astype(BF16)

        gates[mine, span] = silu_of_twice(
            jnp.dot(hot[u, pl.ds(HALO, events), :], tgate[:, span], preferred_element_type=F32)
        )
        base = pl.multiple_of(s * STRETCH, STRETCH)
        place_rows = pl.ds(pl.multiple_of(u * events + s * STRETCH, STRETCH), STRETCH)
        seen = outward[place_rows, :]
        scores = jnp.dot(
            seen, inward_t[u, :, pl.ds(base, STRETCH)], preferred_element_type=F32
        )
        scores = jnp.where(causal, scores, 0.0)
        known = facts[place_rows, :]
        wide_seen = seen.astype(F32)
        for p in range(heads):
            h = head_of(p)
            gap = jnp.minimum(logs_t[u, s, p : p + 1, :] - known[:, p : p + 1], 0.0)
            weights = (jnp.exp(gap) * (scores * steps_t[u, s, p : p + 1, :])).astype(BF16)
            faded = (wide_seen * known[:, 2 * heads + p : 2 * heads + p + 1]).astype(BF16)
            q = p % rows
            right = jnp.concatenate(
                [
                    signal[u, p, pl.ds(base, STRETCH), :],
                    held[u * per + p // rows, s, :, q * LANES : (q + 1) * LANES],
                ],
                axis=0,
            )
            y[place_rows, h * LANES : (h + 1) * LANES] = jnp.dot(
                jnp.concatenate([weights, faded], axis=1), right, preferred_element_type=F32
            )
        return now

    done = lax.fori_loop(0, ticks, local_step, (0, 0))
    lax.fori_loop(done[0], pieces, gather_piece, 0)
    lax.fori_loop(done[1], pieces, enter_piece, 0)
    for p in range(heads):
        wout_copy(p).wait()

    def finish_step(u, carry):
        def rows_of(i):
            return pl.ds(pl.multiple_of(u * events + i * tall, tall), tall)

        for j in range(per):
            base = (u * per + j) * parts
            for i in range(parts):
                for d in range(1, rows):
                    enter_copy(base + i, d).wait_recv()
            for i in range(events // tall):
                span = rows_of(i)
                squares = None
                for q in range(0, rows, 2):
                    pair = range(q, min(q + 2, rows))
                    state = [
                        jnp.concatenate([enter[base + n, e] for n in range(parts)], axis=0)
                        for e in pair
                    ]
                    far = jnp.dot(
                        outward[span, :],
                        jnp.concatenate(state, axis=1),
                        preferred_element_type=F32,
                    )
                    for e in pair:
                        h = e * per + j
                        p = j * rows + e
                        where = slice(h * LANES, (h + 1) * LANES)
                        part = far[:, (e - q) * LANES : (e - q + 1) * LANES]
                        fade = facts[span, 3 * heads + p : 3 * heads + p + 1]
                        value = (y[span, where] + part * fade) * gates[span, where]
                        mix[i, :, e * LANES : (e + 1) * LANES] = (value * gain_ref[:, where]).astype(BF16)
                        squares = value * value if squares is None else squares + value * value
                product = jnp.dot(
                    mix[i],
                    wout[j * wide_group : (j + 1) * wide_group, :],
                    preferred_element_type=F32,
                )
                if j > 0:
                    squares = squares + sums[i]
                    product = product + partial[i]
                if j < per - 1:
                    sums[i] = squares
                    partial[i] = product
                else:
                    mean = jnp.sum(squares, axis=1, keepdims=True) * (1.0 / inner)
                    scale = lax.rsqrt(mean + 1.0) * facts[span, 4 * heads : 4 * heads + 1]
                    out_ref[span, :] = (product * scale).astype(BF16)
        return carry

    lax.fori_loop(0, users, finish_step, 0)

    @pl.when(has_after)
    def _():
        halo_copy.wait_send()

    for u in range(users):
        for d in range(1, rows):
            log_copy(u, d).wait_send()
    for k in range(pieces):
        for d in range(1, rows):
            state_copy(k, d).wait_send()
            enter_copy(k, d).wait_send()
    if cols > 1:

        @pl.when(c < cols - 1)
        def _():
            for k in range(pieces):
                near_copy(k).wait_send()

        @pl.when(gives_own)
        def _():
            for k in range(pieces):
                fade_copy(k).wait_send()

        @pl.when(gives_far)
        def _():
            for k in range(pieces):
                far_copy(k).wait_send()


def per_device(
    item_ids,
    pad_masks,
    lengths,
    item_table,
    w_gate,
    w_in,
    w_dt,
    conv_taps,
    dt_bias,
    decay_rates,
    norm_gain,
    w_out,
):
    users, _, events = item_ids.shape
    items, model = item_table.shape
    full_width = w_in.shape[1]
    inner = w_gate.shape[1]
    heads = decay_rates.shape[0]
    state_width = (full_width - inner) // 2
    rows, cols = lax.axis_size("row"), lax.axis_size("col")
    stretches = events // STRETCH
    per = heads // rows
    parts = 1
    pieces = users * per * parts
    total = users * events
    tall = 2 * STRETCH if events % (2 * STRETCH) == 0 else STRETCH
    group = rows * LANES
    head = (state_width // parts, LANES)

    vmem = pl.BlockSpec(memory_space=pltpu.VMEM)
    hbm = pl.BlockSpec(memory_space=pltpu.HBM)
    dma = pltpu.SemaphoreType.DMA

    def f32(*shape):
        return pltpu.VMEM(shape, F32)

    def bf16(*shape):
        return pltpu.VMEM(shape, BF16)

    result = pl.pallas_call(
        functools.partial(mixer_kernel, (rows, cols, users, heads, tall, parts)),
        in_specs=[hbm] * 12,
        out_specs=vmem,
        out_shape=jax.ShapeDtypeStruct((total, w_out.shape[1]), BF16),
        scratch_shapes=[
            pltpu.SMEM(lengths.shape, jnp.int32),
            pltpu.VMEM(item_ids.shape, jnp.int32),
            pltpu.VMEM(pad_masks.shape, jnp.int32),
            bf16(*w_dt.shape[::-1]),
            f32(*conv_taps.shape),
            f32(1, heads),
            f32(1, heads),
            f32(1, inner),
            bf16(items, model),
            bf16(model, full_width),
            bf16(model, inner),
            bf16(*w_out.shape),
            bf16(items, full_width),
            bf16(items, inner),
            bf16(4 * heads, items),
            bf16(2 * heads, model),
            f32(2, heads, LANES),
            f32(heads + 2, 8, LANES),
            bf16(users, HALO + events, items),
            f32(heads + 2, HALO + events, LANES),
            bf16(users, state_width, events),
            bf16(total, state_width),
            f32(total, LANES),
            f32(users, stretches, heads, LANES),
            f32(users, stretches, heads, LANES),
            f32(users * per, stretches, 8, group),
            bf16(users, heads, events, LANES),
            bf16(per, events, group),
            bf16(users * per, stretches, state_width, group),
            bf16(pieces, rows, *head),
            bf16(pieces, rows, *head),
            f32(users, rows, per, 8, LANES),
            f32(users, rows, per, 8, LANES),
            f32(pieces, rows + 1, *head),
            f32(pieces, rows + 1, 8, LANES),
            f32(*head),
            bf16(pieces, *head),
            bf16(pieces, *head),
            f32(pieces, 8, LANES),
            bf16(pieces, *head),
            f32(pieces, 8, LANES),
            bf16(pieces, rows, *head),
            bf16(pieces, rows, *head),
            f32(total, inner),
            f32(total, inner),
            bf16(events // tall, tall, group),
            f32(events // tall, tall, LANES),
            f32(events // tall, tall, w_out.shape[1]),
            pltpu.VMEM((users, 1, STRETCH), jnp.int32),
            dma((2 * heads + 4,)),
            dma((8,)),
            dma((2,)),
            dma((users, rows)),
            dma((users, rows)),
            dma((pieces, rows)),
            dma((pieces, rows)),
            dma((pieces,)),
            dma((pieces,)),
            dma((pieces, rows)),
            dma((pieces, rows)),
            dma((pieces,)),
            dma((pieces,)),
            dma((pieces,)),
            dma((pieces,)),
        ],
        compiler_params=pltpu.CompilerParams(
            collective_id=0, has_side_effects=True, vmem_limit_bytes=48 * 1024 * 1024
        ),
        name="mixer",
    )(
        *(
            pltpu.with_memory_space_constraint(array, pltpu.HBM)
            for array in (
                lengths,
                item_ids,
                pad_masks,
                w_dt.T,
                conv_taps,
                dt_bias[None],
                decay_rates[None],
                norm_gain[None],
                item_table,
                w_in,
                w_gate,
                w_out,
            )
        )
    )
    return result.reshape(users, 1, events, -1)


def solution(mesh):
    in_specs = (
        P("batch", "col", "row"),
        P("batch", "col", "row"),
        P("batch"),
        P(),
        P(),
        P(),
        P(),
        P(),
        P(),
        P(),
        P(),
        P(),
    )
    out_specs = P("batch", "col", "row", None)
    return jax.shard_map(
        per_device, mesh=mesh, in_specs=in_specs, out_specs=out_specs, check_vma=False
    )
```

```python
import functools

import jax
import jax.numpy as jnp
from jax import lax
from jax.experimental import pallas as pl
from jax.experimental.pallas import tpu as pltpu
from jax.sharding import PartitionSpec as P

STRETCH = 128
LANES = 128
HALO = 16
MESH = pl.DeviceIdType.MESH
F32 = jnp.float32
BF16 = jnp.bfloat16


def silu_of_twice(half):
    return half * (1.0 + jnp.tanh(half))


def remote(src, dst, send, recv, device):
    return pltpu.make_async_remote_copy(
        src_ref=src,
        dst_ref=dst,
        send_sem=send,
        recv_sem=recv,
        device_id=device,
        device_id_type=MESH,
    )


def mixer_kernel(
    counts,
    lengths_hbm,
    ids_hbm,
    masks_hbm,
    wdt_hbm,
    taps_hbm,
    bias_hbm,
    rates_hbm,
    gain_hbm,
    table_hbm,
    win_hbm,
    wgate_hbm,
    wout_hbm,
    out_ref,
    lengths_ref,
    ids_ref,
    masks_ref,
    wdt_ref,
    taps_ref,
    bias_ref,
    rates_ref,
    gain_ref,
    table,
    win,
    wgate,
    wout,
    tin,
    tgate,
    tdt,
    wide,
    params,
    ptaps,
    hot,
    rowbuf,
    inward_t,
    outward,
    facts,
    logs_t,
    steps_t,
    shrinks,
    signal,
    scaled,
    held,
    ssend,
    rin,
    aft,
    lin,
    before,
    fades,
    pin,
    nearin,
    farin,
    fadein,
    psend,
    qsend,
    fsend,
    esend,
    enter,
    y,
    gates,
    mix,
    sums,
    partial,
    landed,
    wsem,
    psem,
    hsem,
    lsem_s,
    lsem_r,
    s1,
    r1,
    s2,
    r2,
    s3,
    r3,
    s4,
    r4,
    s5,
    r5,
):
    rows, cols, users, heads, tall, parts = counts
    events = ids_ref.shape[2]
    stretches = events // STRETCH
    kernel = taps_ref.shape[0]
    inner = wgate.shape[1]
    per = heads // rows
    pieces = users * per * parts
    piece_rows = nearin.shape[1]
    wide_group = rows * LANES
    r, c = lax.axis_index("row"), lax.axis_index("col")
    place = c * rows + r
    places = rows * cols
    later = lax.rem(place + 1, places)
    earlier = lax.rem(place + places - 1, places)
    after = {"row": lax.rem(later, rows), "col": later // rows}
    ahead = {"row": lax.rem(earlier, rows), "col": earlier // rows}
    has_after, has_before = place < places - 1, place > 0
    wraps = jnp.logical_and(r == rows - 1, c < cols - 1)
    wrapped = jnp.logical_and(r == 0, c > 0)

    def head_of(p):
        return (p % rows) * per + p // rows

    win_parts = 4
    win_rows = win.shape[0] // win_parts

    def win_copy(i):
        lines = pl.ds(i * win_rows, win_rows)
        return pltpu.make_async_copy(win_hbm.at[lines, :], win.at[lines, :], wsem.at[i])

    blocks = heads + 2
    table_copy = pltpu.make_async_copy(table_hbm, table, wsem.at[blocks])
    wgate_copy = pltpu.make_async_copy(wgate_hbm, wgate, wsem.at[blocks + 1])

    def wout_copy(p):
        return pltpu.make_async_copy(
            wout_hbm.at[pl.ds(head_of(p) * LANES, LANES), :],
            wout.at[pl.ds(p * LANES, LANES), :],
            wsem.at[blocks + 2 + p],
        )
    small = [
        pltpu.make_async_copy(source, target, psem.at[i])
        for i, (source, target) in enumerate(
            (
                (ids_hbm, ids_ref),
                (masks_hbm, masks_ref),
                (lengths_hbm, lengths_ref),
                (wdt_hbm, wdt_ref),
                (taps_hbm, taps_ref),
                (bias_hbm, bias_ref),
                (rates_hbm, rates_ref),
                (gain_hbm, gain_ref),
            )
        )
    ]
    for copy in small:
        copy.start()
    table_copy.start()
    for i in range(win_parts):
        win_copy(i).start()

    barrier = pltpu.get_barrier_semaphore()
    for d in range(1, rows):
        pl.semaphore_signal(
            barrier, inc=1, device_id={"row": lax.rem(r + d, rows)}, device_id_type=MESH
        )

    @pl.when(c > 0)
    def _():
        pl.semaphore_signal(barrier, inc=1, device_id={"col": c - 1}, device_id_type=MESH)

    @pl.when(c < cols - 1)
    def _():
        pl.semaphore_signal(barrier, inc=1, device_id={"col": c + 1}, device_id_type=MESH)

    @pl.when(c > 1)
    def _():
        pl.semaphore_signal(barrier, inc=1, device_id={"col": c - 2}, device_id_type=MESH)

    @pl.when(c < cols - 2)
    def _():
        pl.semaphore_signal(barrier, inc=1, device_id={"col": c + 2}, device_id_type=MESH)

    @pl.when(wraps)
    def _():
        pl.semaphore_signal(barrier, inc=1, device_id=after, device_id_type=MESH)

    @pl.when(wrapped)
    def _():
        pl.semaphore_signal(barrier, inc=1, device_id=ahead, device_id_type=MESH)

    halo_copy = remote(
        ids_ref.at[:, :, pl.ds(events - STRETCH, STRETCH)], landed, hsem.at[0], hsem.at[1], after
    )

    wide[...] = jnp.zeros_like(wide)
    for copy in small:
        copy.wait()
    def mark_items(u, ids, skip, first, count):
        names = jnp.transpose(jnp.broadcast_to(ids.astype(F32), (8, ids.shape[1])))
        names = names[skip:, 0:1].astype(jnp.int32)
        lane = lax.broadcasted_iota(jnp.int32, (count, table.shape[0]), 1)
        hot[u, first : first + count, :] = (names == lane).astype(F32).astype(BF16)

    def mark_step(u, carry):
        mark_items(u, ids_ref[u], 0, HALO, events)
        return carry

    lax.fori_loop(0, users, mark_step, 0)

    peers = (
        rows
        - 1
        + jnp.where(c > 0, 1, 0)
        + jnp.where(c < cols - 1, 1, 0)
        + jnp.where(c > 1, 1, 0)
        + jnp.where(c < cols - 2, 1, 0)
        + jnp.where(wraps, 1, 0)
        + jnp.where(wrapped, 1, 0)
    )
    pl.semaphore_wait(barrier, peers)

    @pl.when(has_after)
    def _():
        halo_copy.start()

    line_rows = lax.broadcasted_iota(jnp.int32, (STRETCH, STRETCH), 0)
    line_cols = lax.broadcasted_iota(jnp.int32, (STRETCH, STRETCH), 1)
    causal = line_rows >= line_cols
    for i, source in enumerate((bias_ref, rates_ref)):
        value = jnp.zeros((heads, LANES), F32)
        for p in range(heads):
            value = jnp.where(line_rows[0:heads] == p, source[:, head_of(p) : head_of(p) + 1], value)
        params[i] = value
    wide[0:heads, :] = jnp.concatenate(
        [wdt_ref[head_of(p) : head_of(p) + 1, :] for p in range(heads)], axis=0
    )
    for p in range(blocks):
        source = p if p >= heads else head_of(p)
        scale = 0.5 if p < heads else 1.0
        ptaps[p, 0:kernel, :] = scale * taps_ref[:, source * LANES : (source + 1) * LANES]

    table_copy.wait()

    for i in range(win_parts):
        win_copy(i).wait()

    def table_pair(first, left, right):
        weights = jnp.concatenate([win[:, left], win[:, right]], axis=1)
        tin[:, pl.ds(first, 2 * LANES)] = jnp.dot(
            table[...], weights, preferred_element_type=F32
        ).astype(BF16)

    table_pair(
        heads * LANES,
        slice(heads * LANES, (heads + 1) * LANES),
        slice((heads + 1) * LANES, (heads + 2) * LANES),
    )

    raw = lax.dot_general(
        wide[...], table[...], (((1,), (1,)), ((), ())), preferred_element_type=F32
    )[0:heads]
    high = raw.astype(BF16).astype(F32)
    middle = (raw - high).astype(BF16).astype(F32)
    low = raw - high - middle
    tdt[...] = jnp.concatenate([high, middle, low, jnp.zeros_like(low)], axis=0).astype(BF16)

    for i in range(heads // 2):
        table_pair(
            i * 2 * LANES,
            *(
                slice(head_of(p) * LANES, (head_of(p) + 1) * LANES)
                for p in (2 * i, 2 * i + 1)
            ),
        )
    wgate_copy.start()
    for p in range(heads):
        wout_copy(p).start()

    @pl.when(place == 0)
    def _():
        landed[...] = jnp.full(landed.shape, -1, jnp.int32)

    @pl.when(has_before)
    def _():
        halo_copy.wait_recv()

    def convolve(position):
        total = None
        for k in range(kernel):
            part = rowbuf[position, pl.ds(HALO - kernel + 1 + k, events), :] * ptaps[position, k : k + 1, :]
            total = part if total is None else total + part
        return total

    def log_copy(u, d):
        q = lax.rem(r + d, rows)
        return remote(
            aft.at[u, q], lin.at[u, r], lsem_s.at[u, d], lsem_r.at[u, d], {"row": q}
        )

    def state_copy(k, d):
        q = lax.rem(r + d, rows)
        return remote(ssend.at[k, q], rin.at[k, r], s1.at[k, d], r1.at[k, d], {"row": q})

    def near_copy(k):
        return remote(
            psend.at[k], nearin.at[k], s2.at[k], r2.at[k], {"col": lax.rem(c + 1, cols)}
        )

    def fade_copy(k):
        return remote(
            fsend.at[k], fadein.at[k], s4.at[k], r4.at[k], {"col": lax.rem(c + 1, cols)}
        )

    def far_copy(k):
        return remote(
            qsend.at[k], farin.at[k], s5.at[k], r5.at[k], {"col": lax.rem(c + 2, cols)}
        )

    def enter_copy(k, d):
        q = lax.rem(r + d, rows)
        return remote(esend.at[k, q], enter.at[k, r], s3.at[k, d], r3.at[k, d], {"row": q})

    def prepare(u):
        first = place * events
        position = first + lax.broadcasted_iota(jnp.int32, (1, events), 1)
        kept = jnp.where(position < lengths_ref[u], masks_ref[u], 0)
        kept = jnp.where(kept > 0, 1.0, 0.0).astype(F32)
        mark_items(u, landed[u], STRETCH - HALO, 0, HALO)
        shares = lax.dot_general(
            tdt[...],
            hot[u, pl.ds(HALO, events), :],
            (((1,), (1,)), ((), ())),
            preferred_element_type=F32,
        )
        gather_pair(u, heads // 2)
        gather_pair(u, 0)
        raw = shares[0:heads] + shares[heads : 2 * heads] + shares[2 * heads : 3 * heads]
        upper = jnp.where(line_rows <= line_cols, 1.0, 0.0).astype(F32)
        steps, paced = [], []
        for s in range(stretches):
            span = slice(s * STRETCH, (s + 1) * STRETCH)
            value = raw[:, span] + params[0]
            step = kept[:, span] * (jnp.maximum(value, 0.0) + jnp.log1p(jnp.exp(-jnp.abs(value))))
            steps.append(step)
            paced.append(step * params[1])
        sums = jnp.dot(
            jnp.concatenate(paced, axis=0),
            upper,
            precision=lax.Precision.HIGHEST,
            preferred_element_type=F32,
        )
        past = jnp.zeros((heads, LANES), F32)
        for s in range(stretches):
            log = sums[s * heads : (s + 1) * heads]
            step = steps[s]
            logs_t[u, s] = log
            steps_t[u, s] = step
            total = jnp.broadcast_to(log[:, STRETCH - 1 :], (heads, LANES))
            tail = jnp.exp(log - total) * step
            shrink = jnp.exp(-total)
            for p in range(heads):
                shrinks[u * per + p // rows, s, :, (p % rows) * LANES : (p % rows + 1) * LANES] = (
                    jnp.broadcast_to(shrink[p : p + 1], (8, LANES))
                )
            used = jnp.broadcast_to(kept[:, s * STRETCH : (s + 1) * STRETCH], (heads, LANES))
            facts[pl.ds(pl.multiple_of(u * events + s * STRETCH, STRETCH), STRETCH), :] = jnp.transpose(
                jnp.concatenate(
                    [log, tail, jnp.exp(-log), jnp.exp(-(log + past)), used]
                    + [jnp.zeros((LANES - 5 * heads, LANES), F32)],
                    axis=0,
                )
            )
            past = past + total
        for p in range(heads):
            aft[u, p % rows, p // rows] = jnp.broadcast_to(past[p : p + 1], (8, LANES))
        inward_t[u] = jnp.transpose(convolve(heads)).astype(BF16)
        outward[pl.ds(pl.multiple_of(u * events, events), events), :] = convolve(heads + 1).astype(BF16)
        for d in range(1, rows):
            log_copy(u, d).start()
        lin[u, r] = aft[u, r]

    def gather_pair(u, a):
        both = jnp.dot(
            hot[u], tin[:, 2 * a * LANES : 2 * (a + 1) * LANES], preferred_element_type=F32
        )
        rowbuf[2 * a] = both[:, :LANES]
        rowbuf[2 * a + 1] = both[:, LANES:]

    def convert(u, p):
        mine = pl.ds(pl.multiple_of(u * events, events), events)
        j, q = p // rows, p % rows
        value = silu_of_twice(convolve(p)).astype(BF16)
        signal[u, p] = value
        scaled[j, :, q * LANES : (q + 1) * LANES] = (
            value.astype(F32) * facts[mine, heads + p : heads + p + 1]
        ).astype(BF16)

    def form_state(u, j):
        k = u * per + j
        run = None
        for s in range(stretches):
            span = slice(s * STRETCH, (s + 1) * STRETCH)
            added = jnp.dot(
                inward_t[u, :, span], scaled[j, span, :], preferred_element_type=F32
            )
            if run is None:
                held[k, s] = jnp.zeros_like(held[k, s])
                run = added
            else:
                held[k, s] = run.astype(BF16)
                run = run * shrinks[k, s, 0:1, :] + added
        for i in range(parts):
            lines = slice(i * piece_rows, (i + 1) * piece_rows)
            for q in range(rows):
                ssend[k * parts + i, q] = run[lines, q * LANES : (q + 1) * LANES].astype(BF16)
            for d in range(1, rows):
                state_copy(k * parts + i, d).start()

    def user_step(u, carry):
        prepare(u)
        for a in range(heads // 2):
            if a + 1 < heads // 2:
                gather_pair(u, a + 1)
            convert(u, 2 * a)
            convert(u, 2 * a + 1)
            for j in range(per):
                if 2 * a < (j + 1) * rows <= 2 * a + 2:
                    form_state(u, j)
        return carry

    lax.fori_loop(0, users, user_step, 0)

    gives_near = c < cols - 1
    gives_far = c < cols - 2

    def gather_piece(k, carry):
        u, j = k // (per * parts), lax.rem(k // parts, per)
        rin[k, r] = ssend[k, r]

        @pl.when(lax.rem(k, per * parts) == 0)
        def _():
            for d in range(1, rows):
                log_copy(u, d).wait_recv()

        for d in range(1, rows):
            state_copy(k, d).wait_recv()
        carried = jnp.zeros(nearin.shape[1:], F32)
        fade = jnp.ones((8, LANES), F32)
        for m in range(rows):
            before[k, m] = carried
            fades[k, m] = fade
            here = jnp.exp(-lin[u, m, j])
            carried = here[0:1] * carried + rin[k, m].astype(F32)
            fade = fade * here
        before[k, rows] = carried
        fades[k, rows] = fade
        if cols > 1:

            @pl.when(gives_near)
            def _():
                psend[k] = carried.astype(BF16)
                fsend[k] = fade
                near_copy(k).start()
                fade_copy(k).start()

        return carry

    def enter_piece(k, carry):
        @pl.when(c == 0)
        def _():
            pin[...] = jnp.zeros_like(pin)

        if cols > 1:

            @pl.when(c > 0)
            def _():
                near_copy(k).wait_recv()
                fade_copy(k).wait_recv()
                pin[...] = nearin[k].astype(F32)

            @pl.when(c > 1)
            def _():
                far_copy(k).wait_recv()
                pin[...] = fadein[k, 0:1] * farin[k].astype(F32) + nearin[k].astype(F32)

            @pl.when(gives_far)
            def _():
                qsend[k] = (fades[k, rows, 0:1] * pin[...] + before[k, rows]).astype(BF16)
                far_copy(k).start()

        for q in range(rows):
            esend[k, q] = (fades[k, q, 0:1] * pin[...] + before[k, q]).astype(BF16)
        for d in range(1, rows):
            enter_copy(k, d).start()
        enter[k, r] = esend[k, r]
        return carry

    ticks = users * stretches

    marks = [u * stretches + (j if u == 0 else 0) for u in range(users) for j in range(per)]

    def due(t):
        return sum(jnp.where(t >= mark, 1, 0) for mark in marks)

    lag = jnp.maximum(2 * c - 1, 0)

    wgate_copy.wait()
    chunk = inner // stretches

    def local_step(t, done):
        now = due(t), due(t - lag)
        lax.fori_loop(done[0], now[0], gather_piece, 0)
        lax.fori_loop(done[1], now[1], enter_piece, 0)
        u, s = t // stretches, lax.rem(t, stretches)
        span = pl.ds(pl.multiple_of(s * chunk, chunk), chunk)
        mine = pl.ds(pl.multiple_of(u * events, events), events)

        @pl.when(u == 0)
        def _():
            tgate[:, span] = (
                0.5 * jnp.dot(table[...], wgate[:, span], preferred_element_type=F32)
            ).astype(BF16)

        gates[mine, span] = silu_of_twice(
            jnp.dot(hot[u, pl.ds(HALO, events), :], tgate[:, span], preferred_element_type=F32)
        )
        base = pl.multiple_of(s * STRETCH, STRETCH)
        place_rows = pl.ds(pl.multiple_of(u * events + s * STRETCH, STRETCH), STRETCH)
        seen = outward[place_rows, :]
        scores = jnp.dot(
            seen, inward_t[u, :, pl.ds(base, STRETCH)], preferred_element_type=F32
        )
        scores = jnp.where(causal, scores, 0.0)
        known = facts[place_rows, :]
        wide_seen = seen.astype(F32)
        for p in range(heads):
            h = head_of(p)
            gap = jnp.minimum(logs_t[u, s, p : p + 1, :] - known[:, p : p + 1], 0.0)
            weights = (jnp.exp(gap) * (scores * steps_t[u, s, p : p + 1, :])).astype(BF16)
            faded = (wide_seen * known[:, 2 * heads + p : 2 * heads + p + 1]).astype(BF16)
            q = p % rows
            right = jnp.concatenate(
                [
                    signal[u, p, pl.ds(base, STRETCH), :],
                    held[u * per + p // rows, s, :, q * LANES : (q + 1) * LANES],
                ],
                axis=0,
            )
            y[place_rows, h * LANES : (h + 1) * LANES] = jnp.dot(
                jnp.concatenate([weights, faded], axis=1), right, preferred_element_type=F32
            )
        return now

    done = lax.fori_loop(0, ticks, local_step, (0, 0))
    lax.fori_loop(done[0], pieces, gather_piece, 0)
    lax.fori_loop(done[1], pieces, enter_piece, 0)
    for p in range(heads):
        wout_copy(p).wait()

    def finish_step(u, carry):
        def rows_of(i):
            return pl.ds(pl.multiple_of(u * events + i * tall, tall), tall)

        for j in range(per):
            base = (u * per + j) * parts
            for i in range(parts):
                for d in range(1, rows):
                    enter_copy(base + i, d).wait_recv()
            for i in range(events // tall):
                span = rows_of(i)
                squares = None
                for q in range(0, rows, 2):
                    pair = range(q, min(q + 2, rows))
                    state = [
                        jnp.concatenate([enter[base + n, e] for n in range(parts)], axis=0)
                        for e in pair
                    ]
                    far = jnp.dot(
                        outward[span, :],
                        jnp.concatenate(state, axis=1),
                        preferred_element_type=F32,
                    )
                    for e in pair:
                        h = e * per + j
                        p = j * rows + e
                        where = slice(h * LANES, (h + 1) * LANES)
                        part = far[:, (e - q) * LANES : (e - q + 1) * LANES]
                        fade = facts[span, 3 * heads + p : 3 * heads + p + 1]
                        value = (y[span, where] + part * fade) * gates[span, where]
                        mix[i, :, e * LANES : (e + 1) * LANES] = (value * gain_ref[:, where]).astype(BF16)
                        squares = value * value if squares is None else squares + value * value
                product = jnp.dot(
                    mix[i],
                    wout[j * wide_group : (j + 1) * wide_group, :],
                    preferred_element_type=F32,
                )
                if j > 0:
                    squares = squares + sums[i]
                    product = product + partial[i]
                if j < per - 1:
                    sums[i] = squares
                    partial[i] = product
                else:
                    mean = jnp.sum(squares, axis=1, keepdims=True) * (1.0 / inner)
                    scale = lax.rsqrt(mean + 1.0) * facts[span, 4 * heads : 4 * heads + 1]
                    out_ref[span, :] = (product * scale).astype(BF16)
        return carry

    lax.fori_loop(0, users, finish_step, 0)

    @pl.when(has_after)
    def _():
        halo_copy.wait_send()

    for u in range(users):
        for d in range(1, rows):
            log_copy(u, d).wait_send()
    for k in range(pieces):
        for d in range(1, rows):
            state_copy(k, d).wait_send()
            enter_copy(k, d).wait_send()
    if cols > 1:

        @pl.when(gives_near)
        def _():
            for k in range(pieces):
                near_copy(k).wait_send()
                fade_copy(k).wait_send()

        @pl.when(gives_far)
        def _():
            for k in range(pieces):
                far_copy(k).wait_send()


def per_device(
    item_ids,
    pad_masks,
    lengths,
    item_table,
    w_gate,
    w_in,
    w_dt,
    conv_taps,
    dt_bias,
    decay_rates,
    norm_gain,
    w_out,
):
    users, _, events = item_ids.shape
    items, model = item_table.shape
    full_width = w_in.shape[1]
    inner = w_gate.shape[1]
    heads = decay_rates.shape[0]
    state_width = (full_width - inner) // 2
    rows, cols = lax.axis_size("row"), lax.axis_size("col")
    stretches = events // STRETCH
    per = heads // rows
    parts = 1
    pieces = users * per * parts
    total = users * events
    tall = 2 * STRETCH if events % (2 * STRETCH) == 0 else STRETCH
    group = rows * LANES
    head = (state_width // parts, LANES)

    vmem = pl.BlockSpec(memory_space=pltpu.VMEM)
    hbm = pl.BlockSpec(memory_space=pltpu.HBM)
    dma = pltpu.SemaphoreType.DMA

    def f32(*shape):
        return pltpu.VMEM(shape, F32)

    def bf16(*shape):
        return pltpu.VMEM(shape, BF16)

    result = pl.pallas_call(
        functools.partial(mixer_kernel, (rows, cols, users, heads, tall, parts)),
        in_specs=[hbm] * 12,
        out_specs=vmem,
        out_shape=jax.ShapeDtypeStruct((total, w_out.shape[1]), BF16),
        scratch_shapes=[
            pltpu.SMEM(lengths.shape, jnp.int32),
            pltpu.VMEM(item_ids.shape, jnp.int32),
            pltpu.VMEM(pad_masks.shape, jnp.int32),
            bf16(*w_dt.shape[::-1]),
            f32(*conv_taps.shape),
            f32(1, heads),
            f32(1, heads),
            f32(1, inner),
            bf16(items, model),
            bf16(model, full_width),
            bf16(model, inner),
            bf16(*w_out.shape),
            bf16(items, full_width),
            bf16(items, inner),
            bf16(4 * heads, items),
            bf16(2 * heads, model),
            f32(2, heads, LANES),
            f32(heads + 2, 8, LANES),
            bf16(users, HALO + events, items),
            f32(heads + 2, HALO + events, LANES),
            bf16(users, state_width, events),
            bf16(total, state_width),
            f32(total, LANES),
            f32(users, stretches, heads, LANES),
            f32(users, stretches, heads, LANES),
            f32(users * per, stretches, 8, group),
            bf16(users, heads, events, LANES),
            bf16(per, events, group),
            bf16(users * per, stretches, state_width, group),
            bf16(pieces, rows, *head),
            bf16(pieces, rows, *head),
            f32(users, rows, per, 8, LANES),
            f32(users, rows, per, 8, LANES),
            f32(pieces, rows + 1, *head),
            f32(pieces, rows + 1, 8, LANES),
            f32(*head),
            bf16(pieces, *head),
            bf16(pieces, *head),
            f32(pieces, 8, LANES),
            bf16(pieces, *head),
            bf16(pieces, *head),
            f32(pieces, 8, LANES),
            bf16(pieces, rows, *head),
            bf16(pieces, rows, *head),
            f32(total, inner),
            f32(total, inner),
            bf16(events // tall, tall, group),
            f32(events // tall, tall, LANES),
            f32(events // tall, tall, w_out.shape[1]),
            pltpu.VMEM((users, 1, STRETCH), jnp.int32),
            dma((2 * heads + 4,)),
            dma((8,)),
            dma((2,)),
            dma((users, rows)),
            dma((users, rows)),
            dma((pieces, rows)),
            dma((pieces, rows)),
            dma((pieces,)),
            dma((pieces,)),
            dma((pieces, rows)),
            dma((pieces, rows)),
            dma((pieces,)),
            dma((pieces,)),
            dma((pieces,)),
            dma((pieces,)),
        ],
        compiler_params=pltpu.CompilerParams(
            collective_id=0, has_side_effects=True, vmem_limit_bytes=48 * 1024 * 1024
        ),
        name="mixer",
    )(
        *(
            pltpu.with_memory_space_constraint(array, pltpu.HBM)
            for array in (
                lengths,
                item_ids,
                pad_masks,
                w_dt.T,
                conv_taps,
                dt_bias[None],
                decay_rates[None],
                norm_gain[None],
                item_table,
                w_in,
                w_gate,
                w_out,
            )
        )
    )
    return result.reshape(users, 1, events, -1)


def solution(mesh):
    in_specs = (
        P("batch", "col", "row"),
        P("batch", "col", "row"),
        P("batch"),
        P(),
        P(),
        P(),
        P(),
        P(),
        P(),
        P(),
        P(),
        P(),
    )
    out_specs = P("batch", "col", "row", None)
    return jax.shard_map(
        per_device, mesh=mesh, in_specs=in_specs, out_specs=out_specs, check_vma=False
    )
```

```python
import functools

import jax
import jax.numpy as jnp
from jax import lax
from jax.experimental import pallas as pl
from jax.experimental.pallas import tpu as pltpu
from jax.sharding import PartitionSpec as P

STRETCH = 128
LANES = 128
HALO = 16
MESH = pl.DeviceIdType.MESH
F32 = jnp.float32
BF16 = jnp.bfloat16


def silu_of_twice(half):
    return half * (1.0 + jnp.tanh(half))


def remote(src, dst, send, recv, device):
    return pltpu.make_async_remote_copy(
        src_ref=src,
        dst_ref=dst,
        send_sem=send,
        recv_sem=recv,
        device_id=device,
        device_id_type=MESH,
    )


def mixer_kernel(
    counts,
    lengths_hbm,
    ids_hbm,
    masks_hbm,
    wdt_hbm,
    taps_hbm,
    bias_hbm,
    rates_hbm,
    gain_hbm,
    table_hbm,
    win_hbm,
    wgate_hbm,
    wout_hbm,
    out_ref,
    lengths_ref,
    ids_ref,
    masks_ref,
    wdt_ref,
    taps_ref,
    bias_ref,
    rates_ref,
    gain_ref,
    table,
    win,
    wgate,
    wout,
    tin,
    tgate,
    tdt,
    wide,
    params,
    ptaps,
    hot,
    rowbuf,
    inward_t,
    outward,
    facts,
    logs_t,
    steps_t,
    shrinks,
    signal,
    scaled,
    held,
    ssend,
    rin,
    aft,
    lin,
    before,
    fades,
    pin,
    nearin,
    farin,
    fadein,
    psend,
    qsend,
    fsend,
    esend,
    enter,
    y,
    gates,
    mix,
    sums,
    partial,
    landed,
    wsem,
    psem,
    hsem,
    lsem_s,
    lsem_r,
    s1,
    r1,
    s2,
    r2,
    s3,
    r3,
    s4,
    r4,
    s5,
    r5,
):
    rows, cols, users, heads, tall, parts = counts
    events = ids_ref.shape[2]
    stretches = events // STRETCH
    kernel = taps_ref.shape[0]
    inner = wgate.shape[1]
    per = heads // rows
    pieces = users * per * parts
    piece_rows = nearin.shape[1]
    wide_group = rows * LANES
    r, c = lax.axis_index("row"), lax.axis_index("col")
    place = c * rows + r
    places = rows * cols
    later = lax.rem(place + 1, places)
    earlier = lax.rem(place + places - 1, places)
    after = {"row": lax.rem(later, rows), "col": later // rows}
    ahead = {"row": lax.rem(earlier, rows), "col": earlier // rows}
    has_after, has_before = place < places - 1, place > 0
    wraps = jnp.logical_and(r == rows - 1, c < cols - 1)
    wrapped = jnp.logical_and(r == 0, c > 0)

    def head_of(p):
        return (p % rows) * per + p // rows

    win_parts = 4
    win_rows = win.shape[0] // win_parts

    def win_copy(i):
        lines = pl.ds(i * win_rows, win_rows)
        return pltpu.make_async_copy(win_hbm.at[lines, :], win.at[lines, :], wsem.at[i])

    blocks = heads + 2
    table_copy = pltpu.make_async_copy(table_hbm, table, wsem.at[blocks])
    wgate_copy = pltpu.make_async_copy(wgate_hbm, wgate, wsem.at[blocks + 1])

    def wout_copy(p):
        return pltpu.make_async_copy(
            wout_hbm.at[pl.ds(head_of(p) * LANES, LANES), :],
            wout.at[pl.ds(p * LANES, LANES), :],
            wsem.at[blocks + 2 + p],
        )
    small = [
        pltpu.make_async_copy(source, target, psem.at[i])
        for i, (source, target) in enumerate(
            (
                (ids_hbm, ids_ref),
                (masks_hbm, masks_ref),
                (lengths_hbm, lengths_ref),
                (wdt_hbm, wdt_ref),
                (taps_hbm, taps_ref),
                (bias_hbm, bias_ref),
                (rates_hbm, rates_ref),
                (gain_hbm, gain_ref),
            )
        )
    ]
    for copy in small:
        copy.start()
    table_copy.start()
    for i in range(win_parts):
        win_copy(i).start()

    barrier = pltpu.get_barrier_semaphore()
    for d in range(1, rows):
        pl.semaphore_signal(
            barrier, inc=1, device_id={"row": lax.rem(r + d, rows)}, device_id_type=MESH
        )

    @pl.when(c > 0)
    def _():
        pl.semaphore_signal(barrier, inc=1, device_id={"col": c - 1}, device_id_type=MESH)

    @pl.when(c < cols - 1)
    def _():
        pl.semaphore_signal(barrier, inc=1, device_id={"col": c + 1}, device_id_type=MESH)

    @pl.when(c > 1)
    def _():
        pl.semaphore_signal(barrier, inc=1, device_id={"col": c - 2}, device_id_type=MESH)

    @pl.when(c < cols - 2)
    def _():
        pl.semaphore_signal(barrier, inc=1, device_id={"col": c + 2}, device_id_type=MESH)

    @pl.when(wraps)
    def _():
        pl.semaphore_signal(barrier, inc=1, device_id=after, device_id_type=MESH)

    @pl.when(wrapped)
    def _():
        pl.semaphore_signal(barrier, inc=1, device_id=ahead, device_id_type=MESH)

    halo_copy = remote(
        ids_ref.at[:, :, pl.ds(events - STRETCH, STRETCH)], landed, hsem.at[0], hsem.at[1], after
    )

    wide[...] = jnp.zeros_like(wide)
    for copy in small:
        copy.wait()
    def mark_items(u, ids, skip, first, count):
        names = jnp.transpose(jnp.broadcast_to(ids.astype(F32), (8, ids.shape[1])))
        names = names[skip:, 0:1].astype(jnp.int32)
        lane = lax.broadcasted_iota(jnp.int32, (count, table.shape[0]), 1)
        hot[u, first : first + count, :] = (names == lane).astype(F32).astype(BF16)

    def mark_step(u, carry):
        mark_items(u, ids_ref[u], 0, HALO, events)
        return carry

    lax.fori_loop(0, users, mark_step, 0)

    peers = (
        rows
        - 1
        + jnp.where(c > 0, 1, 0)
        + jnp.where(c < cols - 1, 1, 0)
        + jnp.where(c > 1, 1, 0)
        + jnp.where(c < cols - 2, 1, 0)
        + jnp.where(wraps, 1, 0)
        + jnp.where(wrapped, 1, 0)
    )
    pl.semaphore_wait(barrier, peers)

    @pl.when(has_after)
    def _():
        halo_copy.start()

    line_rows = lax.broadcasted_iota(jnp.int32, (STRETCH, STRETCH), 0)
    line_cols = lax.broadcasted_iota(jnp.int32, (STRETCH, STRETCH), 1)
    causal = line_rows >= line_cols
    for i, source in enumerate((bias_ref, rates_ref)):
        value = jnp.zeros((heads, LANES), F32)
        for p in range(heads):
            value = jnp.where(line_rows[0:heads] == p, source[:, head_of(p) : head_of(p) + 1], value)
        params[i] = value
    wide[0:heads, :] = jnp.concatenate(
        [wdt_ref[head_of(p) : head_of(p) + 1, :] for p in range(heads)], axis=0
    )
    for p in range(blocks):
        source = p if p >= heads else head_of(p)
        scale = 0.5 if p < heads else 1.0
        ptaps[p, 0:kernel, :] = scale * taps_ref[:, source * LANES : (source + 1) * LANES]

    table_copy.wait()

    for i in range(win_parts):
        win_copy(i).wait()

    def table_pair(first, left, right):
        weights = jnp.concatenate([win[:, left], win[:, right]], axis=1)
        tin[:, pl.ds(first, 2 * LANES)] = jnp.dot(
            table[...], weights, preferred_element_type=F32
        ).astype(BF16)

    table_pair(
        heads * LANES,
        slice(heads * LANES, (heads + 1) * LANES),
        slice((heads + 1) * LANES, (heads + 2) * LANES),
    )

    raw = lax.dot_general(
        wide[...], table[...], (((1,), (1,)), ((), ())), preferred_element_type=F32
    )[0:heads]
    high = raw.astype(BF16).astype(F32)
    middle = (raw - high).astype(BF16).astype(F32)
    low = raw - high - middle
    tdt[...] = jnp.concatenate([high, middle, low, jnp.zeros_like(low)], axis=0).astype(BF16)

    for i in range(heads // 2):
        table_pair(
            i * 2 * LANES,
            *(
                slice(head_of(p) * LANES, (head_of(p) + 1) * LANES)
                for p in (2 * i, 2 * i + 1)
            ),
        )
    wgate_copy.start()
    for p in range(heads):
        wout_copy(p).start()

    @pl.when(place == 0)
    def _():
        landed[...] = jnp.full(landed.shape, -1, jnp.int32)

    @pl.when(has_before)
    def _():
        halo_copy.wait_recv()

    def own_rows(u):
        first = u * events
        return pl.ds(first if isinstance(u, int) else pl.multiple_of(first, events), events)

    def convolve(u, position):
        total = None
        for k in range(kernel):
            part = rowbuf[u, position, pl.ds(HALO - kernel + 1 + k, events), :] * ptaps[position, k : k + 1, :]
            total = part if total is None else total + part
        return total

    even = lax.rem(r, 2) == 0
    ends = [jnp.where(even, rows - 1, 1), jnp.where(even, 1, rows - 1)]
    sending_order = [ends[0], *range(2, rows - 1), ends[1]] if rows > 2 else [*range(1, rows)]

    def log_copy(u, d):
        q = lax.rem(r + d, rows)
        return remote(
            aft.at[u, q], lin.at[u, r], lsem_s.at[u, d], lsem_r.at[u, d], {"row": q}
        )

    def state_copy(k, d):
        q = lax.rem(r + d, rows)
        return remote(ssend.at[k, q], rin.at[k, r], s1.at[k, d], r1.at[k, d], {"row": q})

    def near_copy(k):
        return remote(
            psend.at[k], nearin.at[k], s2.at[k], r2.at[k], {"col": lax.rem(c + 1, cols)}
        )

    def fade_copy(k):
        return remote(
            fsend.at[k], fadein.at[k], s4.at[k], r4.at[k], {"col": lax.rem(c + 1, cols)}
        )

    def far_copy(k):
        return remote(
            qsend.at[k], farin.at[k], s5.at[k], r5.at[k], {"col": lax.rem(c + 2, cols)}
        )

    def enter_copy(k, d):
        q = lax.rem(r + d, rows)
        return remote(esend.at[k, q], enter.at[k, r], s3.at[k, d], r3.at[k, d], {"row": q})

    def prepare(u):
        first = place * events
        position = first + lax.broadcasted_iota(jnp.int32, (1, events), 1)
        kept = jnp.where(position < lengths_ref[u], masks_ref[u], 0)
        kept = jnp.where(kept > 0, 1.0, 0.0).astype(F32)
        mark_items(u, landed[u], STRETCH - HALO, 0, HALO)
        shares = lax.dot_general(
            tdt[...],
            hot[u, pl.ds(HALO, events), :],
            (((1,), (1,)), ((), ())),
            preferred_element_type=F32,
        )
        gather_pair(u, heads // 2)
        gather_pair(u, 0)
        raw = shares[0:heads] + shares[heads : 2 * heads] + shares[2 * heads : 3 * heads]
        upper = jnp.where(line_rows <= line_cols, 1.0, 0.0).astype(F32)
        steps, paced = [], []
        for s in range(stretches):
            span = slice(s * STRETCH, (s + 1) * STRETCH)
            value = raw[:, span] + params[0]
            step = kept[:, span] * (jnp.maximum(value, 0.0) + jnp.log1p(jnp.exp(-jnp.abs(value))))
            steps.append(step)
            paced.append(step * params[1])
        sums = jnp.dot(
            jnp.concatenate(paced, axis=0),
            upper,
            precision=lax.Precision.HIGHEST,
            preferred_element_type=F32,
        )
        past = jnp.zeros((heads, LANES), F32)
        for s in range(stretches):
            log = sums[s * heads : (s + 1) * heads]
            step = steps[s]
            logs_t[u, s] = log
            steps_t[u, s] = step
            total = jnp.broadcast_to(log[:, STRETCH - 1 :], (heads, LANES))
            tail = jnp.exp(log - total) * step
            shrink = jnp.exp(-total)
            for p in range(heads):
                shrinks[u * per + p // rows, s, :, (p % rows) * LANES : (p % rows + 1) * LANES] = (
                    jnp.broadcast_to(shrink[p : p + 1], (8, LANES))
                )
            used = jnp.broadcast_to(kept[:, s * STRETCH : (s + 1) * STRETCH], (heads, LANES))
            facts[pl.ds(u * events + s * STRETCH, STRETCH), :] = jnp.transpose(
                jnp.concatenate(
                    [log, tail, jnp.exp(-log), jnp.exp(-(log + past)), used]
                    + [jnp.zeros((LANES - 5 * heads, LANES), F32)],
                    axis=0,
                )
            )
            past = past + total
        for p in range(heads):
            aft[u, p % rows, p // rows] = jnp.broadcast_to(past[p : p + 1], (8, LANES))
        inward_t[u] = jnp.transpose(convolve(u, heads)).astype(BF16)
        outward[own_rows(u), :] = convolve(u, heads + 1).astype(BF16)
        for d in range(1, rows):
            log_copy(u, d).start()
        lin[u, r] = aft[u, r]

    def gather_pair(u, a):
        both = jnp.dot(
            hot[u], tin[:, 2 * a * LANES : 2 * (a + 1) * LANES], preferred_element_type=F32
        )
        rowbuf[u, 2 * a] = both[:, :LANES]
        rowbuf[u, 2 * a + 1] = both[:, LANES:]

    def convert(u, p):
        mine = own_rows(u)
        j, q = p // rows, p % rows
        value = silu_of_twice(convolve(u, p)).astype(BF16)
        signal[u, p] = value
        scaled[u, j, :, q * LANES : (q + 1) * LANES] = (
            value.astype(F32) * facts[mine, heads + p : heads + p + 1]
        ).astype(BF16)

    def form_state(u, j):
        k = u * per + j
        run = None
        for s in range(stretches):
            span = slice(s * STRETCH, (s + 1) * STRETCH)
            added = jnp.dot(
                inward_t[u, :, span], scaled[u, j, span, :], preferred_element_type=F32
            )
            if run is None:
                held[k, s] = jnp.zeros_like(held[k, s])
                run = added
            else:
                held[k, s] = run.astype(BF16)
                run = run * shrinks[k, s, 0:1, :] + added
        for i in range(parts):
            lines = slice(i * piece_rows, (i + 1) * piece_rows)
            for q in range(rows):
                ssend[k * parts + i, q] = run[lines, q * LANES : (q + 1) * LANES].astype(BF16)
            for d in sending_order:
                state_copy(k * parts + i, d).start()

    def user_step(u, carry):
        prepare(u)
        for a in range(heads // 2):
            if a + 1 < heads // 2:
                gather_pair(u, a + 1)
            convert(u, 2 * a)
            convert(u, 2 * a + 1)
            for j in range(per):
                if 2 * a < (j + 1) * rows <= 2 * a + 2:
                    form_state(u, j)
        return carry

    for u in range(users):
        user_step(u, 0)

    gives_near = c < cols - 1
    gives_far = c < cols - 2

    def gather_piece(k, carry):
        u, j = k // (per * parts), lax.rem(k // parts, per)
        rin[k, r] = ssend[k, r]

        @pl.when(lax.rem(k, per * parts) == 0)
        def _():
            for d in range(1, rows):
                log_copy(u, d).wait_recv()

        for d in range(1, rows):
            state_copy(k, d).wait_recv()
        carried = jnp.zeros(nearin.shape[1:], F32)
        fade = jnp.ones((8, LANES), F32)
        for m in range(rows):
            before[k, m] = carried
            fades[k, m] = fade
            here = jnp.exp(-lin[u, m, j])
            carried = here[0:1] * carried + rin[k, m].astype(F32)
            fade = fade * here
        before[k, rows] = carried
        fades[k, rows] = fade
        if cols > 1:

            @pl.when(gives_near)
            def _():
                psend[k] = carried.astype(BF16)
                fsend[k] = fade
                near_copy(k).start()
                fade_copy(k).start()

        return carry

    def enter_piece(k, carry):
        @pl.when(c == 0)
        def _():
            pin[...] = jnp.zeros_like(pin)

        if cols > 1:

            @pl.when(c > 0)
            def _():
                near_copy(k).wait_recv()
                fade_copy(k).wait_recv()
                pin[...] = nearin[k].astype(F32)

            @pl.when(c > 1)
            def _():
                far_copy(k).wait_recv()
                pin[...] = fadein[k, 0:1] * farin[k].astype(F32) + nearin[k].astype(F32)

            @pl.when(gives_far)
            def _():
                qsend[k] = (fades[k, rows, 0:1] * pin[...] + before[k, rows]).astype(BF16)
                far_copy(k).start()

        for q in range(rows):
            esend[k, q] = (fades[k, q, 0:1] * pin[...] + before[k, q]).astype(BF16)
        for d in sending_order:
            enter_copy(k, d).start()
        enter[k, r] = esend[k, r]
        return carry

    ticks = users * stretches

    marks = [u * stretches + (j if u == 0 else 0) for u in range(users) for j in range(per)]

    def due(t):
        return sum(jnp.where(t >= mark, 1, 0) for mark in marks)

    lag = jnp.maximum(2 * c - 1, 0)

    wgate_copy.wait()
    chunk = inner // stretches

    def local_step(t, done):
        now = due(t), due(t - lag)
        lax.fori_loop(done[0], now[0], gather_piece, 0)
        lax.fori_loop(done[1], now[1], enter_piece, 0)
        u, s = t // stretches, lax.rem(t, stretches)
        span = pl.ds(pl.multiple_of(s * chunk, chunk), chunk)
        mine = own_rows(u)

        @pl.when(u == 0)
        def _():
            tgate[:, span] = (
                0.5 * jnp.dot(table[...], wgate[:, span], preferred_element_type=F32)
            ).astype(BF16)

        gates[mine, span] = silu_of_twice(
            jnp.dot(hot[u, pl.ds(HALO, events), :], tgate[:, span], preferred_element_type=F32)
        )
        base = pl.multiple_of(s * STRETCH, STRETCH)
        place_rows = pl.ds(pl.multiple_of(u * events + s * STRETCH, STRETCH), STRETCH)
        seen = outward[place_rows, :]
        scores = jnp.dot(
            seen, inward_t[u, :, pl.ds(base, STRETCH)], preferred_element_type=F32
        )
        scores = jnp.where(causal, scores, 0.0)
        known = facts[place_rows, :]
        wide_seen = seen.astype(F32)
        for p in range(heads):
            h = head_of(p)
            gap = jnp.minimum(logs_t[u, s, p : p + 1, :] - known[:, p : p + 1], 0.0)
            weights = (jnp.exp(gap) * (scores * steps_t[u, s, p : p + 1, :])).astype(BF16)
            faded = (wide_seen * known[:, 2 * heads + p : 2 * heads + p + 1]).astype(BF16)
            q = p % rows
            right = jnp.concatenate(
                [
                    signal[u, p, pl.ds(base, STRETCH), :],
                    held[u * per + p // rows, s, :, q * LANES : (q + 1) * LANES],
                ],
                axis=0,
            )
            y[place_rows, h * LANES : (h + 1) * LANES] = jnp.dot(
                jnp.concatenate([weights, faded], axis=1), right, preferred_element_type=F32
            )
        return now

    done = lax.fori_loop(0, ticks, local_step, (0, 0))
    lax.fori_loop(done[0], pieces, gather_piece, 0)
    lax.fori_loop(done[1], pieces, enter_piece, 0)
    for p in range(heads):
        wout_copy(p).wait()

    def finish_step(u, carry):
        def rows_of(i):
            return pl.ds(pl.multiple_of(u * events + i * tall, tall), tall)

        for j in range(per):
            base = (u * per + j) * parts
            for i in range(parts):
                for d in range(1, rows):
                    enter_copy(base + i, d).wait_recv()
            for i in range(events // tall):
                span = rows_of(i)
                squares = None
                for q in range(0, rows, 2):
                    pair = range(q, min(q + 2, rows))
                    state = [
                        jnp.concatenate([enter[base + n, e] for n in range(parts)], axis=0)
                        for e in pair
                    ]
                    far = jnp.dot(
                        outward[span, :],
                        jnp.concatenate(state, axis=1),
                        preferred_element_type=F32,
                    )
                    for e in pair:
                        h = e * per + j
                        p = j * rows + e
                        where = slice(h * LANES, (h + 1) * LANES)
                        part = far[:, (e - q) * LANES : (e - q + 1) * LANES]
                        fade = facts[span, 3 * heads + p : 3 * heads + p + 1]
                        value = (y[span, where] + part * fade) * gates[span, where]
                        mix[i, :, e * LANES : (e + 1) * LANES] = (value * gain_ref[:, where]).astype(BF16)
                        squares = value * value if squares is None else squares + value * value
                product = jnp.dot(
                    mix[i],
                    wout[j * wide_group : (j + 1) * wide_group, :],
                    preferred_element_type=F32,
                )
                if j > 0:
                    squares = squares + sums[i]
                    product = product + partial[i]
                if j < per - 1:
                    sums[i] = squares
                    partial[i] = product
                else:
                    mean = jnp.sum(squares, axis=1, keepdims=True) * (1.0 / inner)
                    scale = lax.rsqrt(mean + 1.0) * facts[span, 4 * heads : 4 * heads + 1]
                    out_ref[span, :] = (product * scale).astype(BF16)
        return carry

    lax.fori_loop(0, users, finish_step, 0)

    @pl.when(has_after)
    def _():
        halo_copy.wait_send()

    for u in range(users):
        for d in range(1, rows):
            log_copy(u, d).wait_send()
    for k in range(pieces):
        for d in range(1, rows):
            state_copy(k, d).wait_send()
            enter_copy(k, d).wait_send()
    if cols > 1:

        @pl.when(gives_near)
        def _():
            for k in range(pieces):
                near_copy(k).wait_send()
                fade_copy(k).wait_send()

        @pl.when(gives_far)
        def _():
            for k in range(pieces):
                far_copy(k).wait_send()


def per_device(
    item_ids,
    pad_masks,
    lengths,
    item_table,
    w_gate,
    w_in,
    w_dt,
    conv_taps,
    dt_bias,
    decay_rates,
    norm_gain,
    w_out,
):
    users, _, events = item_ids.shape
    items, model = item_table.shape
    full_width = w_in.shape[1]
    inner = w_gate.shape[1]
    heads = decay_rates.shape[0]
    state_width = (full_width - inner) // 2
    rows, cols = lax.axis_size("row"), lax.axis_size("col")
    stretches = events // STRETCH
    per = heads // rows
    parts = 1
    pieces = users * per * parts
    total = users * events
    tall = 2 * STRETCH if events % (2 * STRETCH) == 0 else STRETCH
    group = rows * LANES
    head = (state_width // parts, LANES)

    vmem = pl.BlockSpec(memory_space=pltpu.VMEM)
    hbm = pl.BlockSpec(memory_space=pltpu.HBM)
    dma = pltpu.SemaphoreType.DMA

    def f32(*shape):
        return pltpu.VMEM(shape, F32)

    def bf16(*shape):
        return pltpu.VMEM(shape, BF16)

    result = pl.pallas_call(
        functools.partial(mixer_kernel, (rows, cols, users, heads, tall, parts)),
        in_specs=[hbm] * 12,
        out_specs=vmem,
        out_shape=jax.ShapeDtypeStruct((total, w_out.shape[1]), BF16),
        scratch_shapes=[
            pltpu.SMEM(lengths.shape, jnp.int32),
            pltpu.VMEM(item_ids.shape, jnp.int32),
            pltpu.VMEM(pad_masks.shape, jnp.int32),
            bf16(*w_dt.shape[::-1]),
            f32(*conv_taps.shape),
            f32(1, heads),
            f32(1, heads),
            f32(1, inner),
            bf16(items, model),
            bf16(model, full_width),
            bf16(model, inner),
            bf16(*w_out.shape),
            bf16(items, full_width),
            bf16(items, inner),
            bf16(4 * heads, items),
            bf16(2 * heads, model),
            f32(2, heads, LANES),
            f32(heads + 2, 8, LANES),
            bf16(users, HALO + events, items),
            f32(users, heads + 2, HALO + events, LANES),
            bf16(users, state_width, events),
            bf16(total, state_width),
            f32(total, LANES),
            f32(users, stretches, heads, LANES),
            f32(users, stretches, heads, LANES),
            f32(users * per, stretches, 8, group),
            bf16(users, heads, events, LANES),
            bf16(users, per, events, group),
            bf16(users * per, stretches, state_width, group),
            bf16(pieces, rows, *head),
            bf16(pieces, rows, *head),
            f32(users, rows, per, 8, LANES),
            f32(users, rows, per, 8, LANES),
            f32(pieces, rows + 1, *head),
            f32(pieces, rows + 1, 8, LANES),
            f32(*head),
            bf16(pieces, *head),
            bf16(pieces, *head),
            f32(pieces, 8, LANES),
            bf16(pieces, *head),
            bf16(pieces, *head),
            f32(pieces, 8, LANES),
            bf16(pieces, rows, *head),
            bf16(pieces, rows, *head),
            f32(total, inner),
            f32(total, inner),
            bf16(events // tall, tall, group),
            f32(events // tall, tall, LANES),
            f32(events // tall, tall, w_out.shape[1]),
            pltpu.VMEM((users, 1, STRETCH), jnp.int32),
            dma((2 * heads + 4,)),
            dma((8,)),
            dma((2,)),
            dma((users, rows)),
            dma((users, rows)),
            dma((pieces, rows)),
            dma((pieces, rows)),
            dma((pieces,)),
            dma((pieces,)),
            dma((pieces, rows)),
            dma((pieces, rows)),
            dma((pieces,)),
            dma((pieces,)),
            dma((pieces,)),
            dma((pieces,)),
        ],
        compiler_params=pltpu.CompilerParams(
            collective_id=0, has_side_effects=True, vmem_limit_bytes=48 * 1024 * 1024
        ),
        name="mixer",
    )(
        *(
            pltpu.with_memory_space_constraint(array, pltpu.HBM)
            for array in (
                lengths,
                item_ids,
                pad_masks,
                w_dt.T,
                conv_taps,
                dt_bias[None],
                decay_rates[None],
                norm_gain[None],
                item_table,
                w_in,
                w_gate,
                w_out,
            )
        )
    )
    return result.reshape(users, 1, events, -1)


def solution(mesh):
    in_specs = (
        P("batch", "col", "row"),
        P("batch", "col", "row"),
        P("batch"),
        P(),
        P(),
        P(),
        P(),
        P(),
        P(),
        P(),
        P(),
        P(),
    )
    out_specs = P("batch", "col", "row", None)
    return jax.shard_map(
        per_device, mesh=mesh, in_specs=in_specs, out_specs=out_specs, check_vma=False
    )
```

```python
import functools

import jax
import jax.numpy as jnp
from jax import lax
from jax.experimental import pallas as pl
from jax.experimental.pallas import tpu as pltpu
from jax.sharding import PartitionSpec as P

STRETCH = 128
LANES = 128
HALO = 16
MESH = pl.DeviceIdType.MESH
F32 = jnp.float32
BF16 = jnp.bfloat16


def silu_of_twice(half):
    return half * (1.0 + jnp.tanh(half))


def remote(src, dst, send, recv, device):
    return pltpu.make_async_remote_copy(
        src_ref=src,
        dst_ref=dst,
        send_sem=send,
        recv_sem=recv,
        device_id=device,
        device_id_type=MESH,
    )


def mixer_kernel(
    counts,
    lengths_hbm,
    ids_hbm,
    masks_hbm,
    wdt_hbm,
    taps_hbm,
    bias_hbm,
    rates_hbm,
    gain_hbm,
    table_hbm,
    win_hbm,
    wgate_hbm,
    wout_hbm,
    out_ref,
    lengths_ref,
    ids_ref,
    masks_ref,
    wdt_ref,
    taps_ref,
    bias_ref,
    rates_ref,
    gain_ref,
    table,
    win,
    wgate,
    wout,
    tin,
    tgate,
    tdt,
    wide,
    params,
    ptaps,
    hot,
    rowbuf,
    inward_t,
    outward,
    facts,
    logs_t,
    steps_t,
    shrinks,
    signal,
    scaled,
    held,
    ssend,
    rin,
    aft,
    lin,
    before,
    fades,
    pin,
    nearin,
    farin,
    fadein,
    psend,
    qsend,
    fsend,
    esend,
    enter,
    y,
    gates,
    mix,
    sums,
    partial,
    landed,
    wsem,
    psem,
    hsem,
    lsem_s,
    lsem_r,
    s1,
    r1,
    s2,
    r2,
    s3,
    r3,
    s4,
    r4,
    s5,
    r5,
):
    rows, cols, users, heads, tall, parts = counts
    events = ids_ref.shape[2]
    stretches = events // STRETCH
    kernel = taps_ref.shape[0]
    inner = wgate.shape[1]
    per = heads // rows
    pieces = users * per * parts
    piece_rows = nearin.shape[1]
    wide_group = rows * LANES
    r, c = lax.axis_index("row"), lax.axis_index("col")
    place = c * rows + r
    places = rows * cols
    later = lax.rem(place + 1, places)
    earlier = lax.rem(place + places - 1, places)
    after = {"row": lax.rem(later, rows), "col": later // rows}
    ahead = {"row": lax.rem(earlier, rows), "col": earlier // rows}
    has_after, has_before = place < places - 1, place > 0
    wraps = jnp.logical_and(r == rows - 1, c < cols - 1)
    wrapped = jnp.logical_and(r == 0, c > 0)

    def head_of(p):
        return (p % rows) * per + p // rows

    win_parts = 4
    win_rows = win.shape[0] // win_parts

    def win_copy(i):
        lines = pl.ds(i * win_rows, win_rows)
        return pltpu.make_async_copy(win_hbm.at[lines, :], win.at[lines, :], wsem.at[i])

    blocks = heads + 2
    table_copy = pltpu.make_async_copy(table_hbm, table, wsem.at[blocks])
    wgate_copy = pltpu.make_async_copy(wgate_hbm, wgate, wsem.at[blocks + 1])

    def wout_copy(p):
        return pltpu.make_async_copy(
            wout_hbm.at[pl.ds(head_of(p) * LANES, LANES), :],
            wout.at[pl.ds(p * LANES, LANES), :],
            wsem.at[blocks + 2 + p],
        )
    small = [
        pltpu.make_async_copy(source, target, psem.at[i])
        for i, (source, target) in enumerate(
            (
                (ids_hbm, ids_ref),
                (masks_hbm, masks_ref),
                (lengths_hbm, lengths_ref),
                (wdt_hbm, wdt_ref),
                (taps_hbm, taps_ref),
                (bias_hbm, bias_ref),
                (rates_hbm, rates_ref),
                (gain_hbm, gain_ref),
            )
        )
    ]
    for copy in small:
        copy.start()
    table_copy.start()
    for i in range(win_parts):
        win_copy(i).start()

    barrier = pltpu.get_barrier_semaphore()
    for d in range(1, rows):
        pl.semaphore_signal(
            barrier, inc=1, device_id={"row": lax.rem(r + d, rows)}, device_id_type=MESH
        )

    @pl.when(c > 0)
    def _():
        pl.semaphore_signal(barrier, inc=1, device_id={"col": c - 1}, device_id_type=MESH)

    @pl.when(c < cols - 1)
    def _():
        pl.semaphore_signal(barrier, inc=1, device_id={"col": c + 1}, device_id_type=MESH)

    @pl.when(c > 1)
    def _():
        pl.semaphore_signal(barrier, inc=1, device_id={"col": c - 2}, device_id_type=MESH)

    @pl.when(c < cols - 2)
    def _():
        pl.semaphore_signal(barrier, inc=1, device_id={"col": c + 2}, device_id_type=MESH)

    @pl.when(wraps)
    def _():
        pl.semaphore_signal(barrier, inc=1, device_id=after, device_id_type=MESH)

    @pl.when(wrapped)
    def _():
        pl.semaphore_signal(barrier, inc=1, device_id=ahead, device_id_type=MESH)

    halo_copy = remote(
        ids_ref.at[:, :, pl.ds(events - STRETCH, STRETCH)], landed, hsem.at[0], hsem.at[1], after
    )

    wide[...] = jnp.zeros_like(wide)
    for copy in small:
        copy.wait()
    def mark_items(u, ids, skip, first, count):
        names = jnp.transpose(jnp.broadcast_to(ids.astype(F32), (8, ids.shape[1])))
        names = names[skip:, 0:1].astype(jnp.int32)
        lane = lax.broadcasted_iota(jnp.int32, (count, table.shape[0]), 1)
        hot[u, first : first + count, :] = (names == lane).astype(F32).astype(BF16)

    def mark_step(u, carry):
        mark_items(u, ids_ref[u], 0, HALO, events)
        return carry

    lax.fori_loop(0, users, mark_step, 0)

    peers = (
        rows
        - 1
        + jnp.where(c > 0, 1, 0)
        + jnp.where(c < cols - 1, 1, 0)
        + jnp.where(c > 1, 1, 0)
        + jnp.where(c < cols - 2, 1, 0)
        + jnp.where(wraps, 1, 0)
        + jnp.where(wrapped, 1, 0)
    )
    pl.semaphore_wait(barrier, peers)

    @pl.when(has_after)
    def _():
        halo_copy.start()

    line_rows = lax.broadcasted_iota(jnp.int32, (STRETCH, STRETCH), 0)
    line_cols = lax.broadcasted_iota(jnp.int32, (STRETCH, STRETCH), 1)
    causal = line_rows >= line_cols
    for i, source in enumerate((bias_ref, rates_ref)):
        value = jnp.zeros((heads, LANES), F32)
        for p in range(heads):
            value = jnp.where(line_rows[0:heads] == p, source[:, head_of(p) : head_of(p) + 1], value)
        params[i] = value
    wide[0:heads, :] = jnp.concatenate(
        [wdt_ref[head_of(p) : head_of(p) + 1, :] for p in range(heads)], axis=0
    )
    for p in range(blocks):
        source = p if p >= heads else head_of(p)
        scale = 0.5 if p < heads else 1.0
        ptaps[p, 0:kernel, :] = scale * taps_ref[:, source * LANES : (source + 1) * LANES]

    table_copy.wait()

    for i in range(win_parts):
        win_copy(i).wait()

    def table_pair(first, left, right):
        weights = jnp.concatenate([win[:, left], win[:, right]], axis=1)
        tin[:, pl.ds(first, 2 * LANES)] = jnp.dot(
            table[...], weights, preferred_element_type=F32
        ).astype(BF16)

    table_pair(
        heads * LANES,
        slice(heads * LANES, (heads + 1) * LANES),
        slice((heads + 1) * LANES, (heads + 2) * LANES),
    )

    raw = lax.dot_general(
        wide[...], table[...], (((1,), (1,)), ((), ())), preferred_element_type=F32
    )[0:heads]
    high = raw.astype(BF16).astype(F32)
    middle = (raw - high).astype(BF16).astype(F32)
    low = raw - high - middle
    tdt[...] = jnp.concatenate([high, middle, low, jnp.zeros_like(low)], axis=0).astype(BF16)

    for i in range(heads // 2):
        table_pair(
            i * 2 * LANES,
            *(
                slice(head_of(p) * LANES, (head_of(p) + 1) * LANES)
                for p in (2 * i, 2 * i + 1)
            ),
        )
    wgate_copy.start()
    for p in range(heads):
        wout_copy(p).start()

    @pl.when(place == 0)
    def _():
        landed[...] = jnp.full(landed.shape, -1, jnp.int32)

    @pl.when(has_before)
    def _():
        halo_copy.wait_recv()

    def own_rows(u):
        first = u * events
        return pl.ds(first if isinstance(u, int) else pl.multiple_of(first, events), events)

    def convolve(u, position):
        total = None
        for k in range(kernel):
            part = rowbuf[u, position, pl.ds(HALO - kernel + 1 + k, events), :] * ptaps[position, k : k + 1, :]
            total = part if total is None else total + part
        return total

    even = lax.rem(r, 2) == 0
    ends = [jnp.where(even, rows - 1, 1), jnp.where(even, 1, rows - 1)]
    sending_order = [ends[0], *range(2, rows - 1), ends[1]] if rows > 2 else [*range(1, rows)]

    def log_copy(u, d):
        q = lax.rem(r + d, rows)
        return remote(
            aft.at[u, q], lin.at[u, r], lsem_s.at[u, d], lsem_r.at[u, d], {"row": q}
        )

    def state_copy(k, d):
        q = lax.rem(r + d, rows)
        return remote(ssend.at[k, q], rin.at[k, r], s1.at[k, d], r1.at[k, d], {"row": q})

    def near_copy(k):
        return remote(
            psend.at[k], nearin.at[k], s2.at[k], r2.at[k], {"col": lax.rem(c + 1, cols)}
        )

    def fade_copy(k):
        return remote(
            fsend.at[k], fadein.at[k], s4.at[k], r4.at[k], {"col": lax.rem(c + 1, cols)}
        )

    def far_copy(k):
        return remote(
            qsend.at[k], farin.at[k], s5.at[k], r5.at[k], {"col": lax.rem(c + 2, cols)}
        )

    def enter_copy(k, d):
        q = lax.rem(r + d, rows)
        return remote(esend.at[k, q], enter.at[k, r], s3.at[k, d], r3.at[k, d], {"row": q})

    def prepare(u):
        first = place * events
        position = first + lax.broadcasted_iota(jnp.int32, (1, events), 1)
        kept = jnp.where(position < lengths_ref[u], masks_ref[u], 0)
        kept = jnp.where(kept > 0, 1.0, 0.0).astype(F32)
        mark_items(u, landed[u], STRETCH - HALO, 0, HALO)
        shares = lax.dot_general(
            tdt[...],
            hot[u, pl.ds(HALO, events), :],
            (((1,), (1,)), ((), ())),
            preferred_element_type=F32,
        )
        gather_pair(u, heads // 2)
        gather_pair(u, 0)
        raw = shares[0:heads] + shares[heads : 2 * heads] + shares[2 * heads : 3 * heads]
        upper = jnp.where(line_rows <= line_cols, 1.0, 0.0).astype(F32)
        steps, paced = [], []
        for s in range(stretches):
            span = slice(s * STRETCH, (s + 1) * STRETCH)
            value = raw[:, span] + params[0]
            step = kept[:, span] * (jnp.maximum(value, 0.0) + jnp.log1p(jnp.exp(-jnp.abs(value))))
            steps.append(step)
            paced.append(step * params[1])
        sums = jnp.dot(
            jnp.concatenate(paced, axis=0),
            upper,
            precision=lax.Precision.HIGHEST,
            preferred_element_type=F32,
        )
        past = jnp.zeros((heads, LANES), F32)
        for s in range(stretches):
            log = sums[s * heads : (s + 1) * heads]
            step = steps[s]
            logs_t[u, s] = log
            steps_t[u, s] = step
            total = jnp.broadcast_to(log[:, STRETCH - 1 :], (heads, LANES))
            tail = jnp.exp(log - total) * step
            shrink = jnp.exp(-total)
            for p in range(heads):
                shrinks[u * per + p // rows, s, :, (p % rows) * LANES : (p % rows + 1) * LANES] = (
                    jnp.broadcast_to(shrink[p : p + 1], (8, LANES))
                )
            used = jnp.broadcast_to(kept[:, s * STRETCH : (s + 1) * STRETCH], (heads, LANES))
            facts[pl.ds(u * events + s * STRETCH, STRETCH), :] = jnp.transpose(
                jnp.concatenate(
                    [log, tail, jnp.exp(-log), jnp.exp(-(log + past)), used]
                    + [jnp.zeros((LANES - 5 * heads, LANES), F32)],
                    axis=0,
                )
            )
            past = past + total
        for p in range(heads):
            aft[u, p % rows, p // rows] = jnp.broadcast_to(past[p : p + 1], (8, LANES))
        inward_t[u] = jnp.transpose(convolve(u, heads)).astype(BF16)
        outward[own_rows(u), :] = convolve(u, heads + 1).astype(BF16)
        for d in range(1, rows):
            log_copy(u, d).start()
        lin[u, r] = aft[u, r]

    def gather_pair(u, a):
        both = jnp.dot(
            hot[u], tin[:, 2 * a * LANES : 2 * (a + 1) * LANES], preferred_element_type=F32
        )
        rowbuf[u, 2 * a] = both[:, :LANES]
        rowbuf[u, 2 * a + 1] = both[:, LANES:]

    def convert(u, p):
        mine = own_rows(u)
        j, q = p // rows, p % rows
        value = silu_of_twice(convolve(u, p)).astype(BF16)
        signal[u, p] = value
        scaled[u, j, :, q * LANES : (q + 1) * LANES] = (
            value.astype(F32) * facts[mine, heads + p : heads + p + 1]
        ).astype(BF16)

    def form_state(u, j):
        k = u * per + j
        run = None
        for s in range(stretches):
            span = slice(s * STRETCH, (s + 1) * STRETCH)
            added = jnp.dot(
                inward_t[u, :, span], scaled[u, j, span, :], preferred_element_type=F32
            )
            if run is None:
                held[k, s] = jnp.zeros_like(held[k, s])
                run = added
            else:
                held[k, s] = run.astype(BF16)
                run = run * shrinks[k, s, 0:1, :] + added
        for i in range(parts):
            lines = slice(i * piece_rows, (i + 1) * piece_rows)
            for q in range(rows):
                ssend[k * parts + i, q] = run[lines, q * LANES : (q + 1) * LANES].astype(BF16)
            for d in sending_order:
                state_copy(k * parts + i, d).start()

    def user_step(u, carry):
        prepare(u)
        for a in range(heads // 2):
            if a + 1 < heads // 2:
                gather_pair(u, a + 1)
            convert(u, 2 * a)
            convert(u, 2 * a + 1)
            for j in range(per):
                if 2 * a < (j + 1) * rows <= 2 * a + 2:
                    form_state(u, j)
        return carry

    for u in range(users):
        user_step(u, 0)

    gives_near = c < cols - 1
    gives_far = c < cols - 2

    def gather_piece(k, carry):
        u, j = k // (per * parts), lax.rem(k // parts, per)
        rin[k, r] = ssend[k, r]

        @pl.when(lax.rem(k, per * parts) == 0)
        def _():
            for d in range(1, rows):
                log_copy(u, d).wait_recv()

        for d in range(1, rows):
            state_copy(k, d).wait_recv()
        carried = jnp.zeros(nearin.shape[1:], F32)
        fade = jnp.ones((8, LANES), F32)
        for m in range(rows):
            before[k, m] = carried
            fades[k, m] = fade
            here = jnp.exp(-lin[u, m, j])
            carried = here[0:1] * carried + rin[k, m].astype(F32)
            fade = fade * here
        before[k, rows] = carried
        fades[k, rows] = fade
        if cols > 1:

            @pl.when(gives_near)
            def _():
                psend[k] = carried.astype(BF16)
                fsend[k] = fade
                near_copy(k).start()
                fade_copy(k).start()

        return carry

    def enter_piece(k, carry):
        @pl.when(c == 0)
        def _():
            pin[...] = jnp.zeros_like(pin)

        if cols > 1:

            @pl.when(c > 0)
            def _():
                near_copy(k).wait_recv()
                fade_copy(k).wait_recv()
                pin[...] = nearin[k].astype(F32)

            @pl.when(c > 1)
            def _():
                far_copy(k).wait_recv()
                pin[...] = fadein[k, 0:1] * farin[k].astype(F32) + nearin[k].astype(F32)

            @pl.when(gives_far)
            def _():
                qsend[k] = (fades[k, rows, 0:1] * pin[...] + before[k, rows]).astype(BF16)
                far_copy(k).start()

        for q in range(rows):
            esend[k, q] = (fades[k, q, 0:1] * pin[...] + before[k, q]).astype(BF16)
        for d in sending_order:
            enter_copy(k, d).start()
        enter[k, r] = esend[k, r]
        return carry

    ticks = users * stretches

    marks = [u * (stretches - 1) + j for u in range(users) for j in range(per)]

    def due(t):
        return sum(jnp.where(t >= mark, 1, 0) for mark in marks)

    lag = jnp.maximum(2 * c - 1, 0)

    wgate_copy.wait()
    chunk = inner // stretches

    def local_step(t, done):
        now = due(t), due(t - lag)
        lax.fori_loop(done[0], now[0], gather_piece, 0)
        lax.fori_loop(done[1], now[1], enter_piece, 0)
        u, s = t // stretches, lax.rem(t, stretches)
        span = pl.ds(pl.multiple_of(s * chunk, chunk), chunk)
        mine = own_rows(u)

        @pl.when(u == 0)
        def _():
            tgate[:, span] = (
                0.5 * jnp.dot(table[...], wgate[:, span], preferred_element_type=F32)
            ).astype(BF16)

        gates[mine, span] = silu_of_twice(
            jnp.dot(hot[u, pl.ds(HALO, events), :], tgate[:, span], preferred_element_type=F32)
        )
        base = pl.multiple_of(s * STRETCH, STRETCH)
        place_rows = pl.ds(pl.multiple_of(u * events + s * STRETCH, STRETCH), STRETCH)
        seen = outward[place_rows, :]
        scores = jnp.dot(
            seen, inward_t[u, :, pl.ds(base, STRETCH)], preferred_element_type=F32
        )
        scores = jnp.where(causal, scores, 0.0)
        known = facts[place_rows, :]
        wide_seen = seen.astype(F32)
        for p in range(heads):
            h = head_of(p)
            gap = jnp.minimum(logs_t[u, s, p : p + 1, :] - known[:, p : p + 1], 0.0)
            weights = (jnp.exp(gap) * (scores * steps_t[u, s, p : p + 1, :])).astype(BF16)
            faded = (wide_seen * known[:, 2 * heads + p : 2 * heads + p + 1]).astype(BF16)
            q = p % rows
            right = jnp.concatenate(
                [
                    signal[u, p, pl.ds(base, STRETCH), :],
                    held[u * per + p // rows, s, :, q * LANES : (q + 1) * LANES],
                ],
                axis=0,
            )
            y[place_rows, h * LANES : (h + 1) * LANES] = jnp.dot(
                jnp.concatenate([weights, faded], axis=1), right, preferred_element_type=F32
            )
        return now

    done = lax.fori_loop(0, ticks, local_step, (0, 0))
    lax.fori_loop(done[0], pieces, gather_piece, 0)
    lax.fori_loop(done[1], pieces, enter_piece, 0)
    for p in range(heads):
        wout_copy(p).wait()

    def finish_step(u, carry):
        def rows_of(i):
            return pl.ds(pl.multiple_of(u * events + i * tall, tall), tall)

        for j in range(per):
            base = (u * per + j) * parts
            for i in range(parts):
                for d in range(1, rows):
                    enter_copy(base + i, d).wait_recv()
            for i in range(events // tall):
                span = rows_of(i)
                squares = None
                for q in range(0, rows, 2):
                    pair = range(q, min(q + 2, rows))
                    state = [
                        jnp.concatenate([enter[base + n, e] for n in range(parts)], axis=0)
                        for e in pair
                    ]
                    far = jnp.dot(
                        outward[span, :],
                        jnp.concatenate(state, axis=1),
                        preferred_element_type=F32,
                    )
                    for e in pair:
                        h = e * per + j
                        p = j * rows + e
                        where = slice(h * LANES, (h + 1) * LANES)
                        part = far[:, (e - q) * LANES : (e - q + 1) * LANES]
                        fade = facts[span, 3 * heads + p : 3 * heads + p + 1]
                        value = (y[span, where] + part * fade) * gates[span, where]
                        mix[i, :, e * LANES : (e + 1) * LANES] = (value * gain_ref[:, where]).astype(BF16)
                        squares = value * value if squares is None else squares + value * value
                product = jnp.dot(
                    mix[i],
                    wout[j * wide_group : (j + 1) * wide_group, :],
                    preferred_element_type=F32,
                )
                if j > 0:
                    squares = squares + sums[i]
                    product = product + partial[i]
                if j < per - 1:
                    sums[i] = squares
                    partial[i] = product
                else:
                    mean = jnp.sum(squares, axis=1, keepdims=True) * (1.0 / inner)
                    scale = lax.rsqrt(mean + 1.0) * facts[span, 4 * heads : 4 * heads + 1]
                    out_ref[span, :] = (product * scale).astype(BF16)
        return carry

    lax.fori_loop(0, users, finish_step, 0)

    @pl.when(has_after)
    def _():
        halo_copy.wait_send()

    for u in range(users):
        for d in range(1, rows):
            log_copy(u, d).wait_send()
    for k in range(pieces):
        for d in range(1, rows):
            state_copy(k, d).wait_send()
            enter_copy(k, d).wait_send()
    if cols > 1:

        @pl.when(gives_near)
        def _():
            for k in range(pieces):
                near_copy(k).wait_send()
                fade_copy(k).wait_send()

        @pl.when(gives_far)
        def _():
            for k in range(pieces):
                far_copy(k).wait_send()


def per_device(
    item_ids,
    pad_masks,
    lengths,
    item_table,
    w_gate,
    w_in,
    w_dt,
    conv_taps,
    dt_bias,
    decay_rates,
    norm_gain,
    w_out,
):
    users, _, events = item_ids.shape
    items, model = item_table.shape
    full_width = w_in.shape[1]
    inner = w_gate.shape[1]
    heads = decay_rates.shape[0]
    state_width = (full_width - inner) // 2
    rows, cols = lax.axis_size("row"), lax.axis_size("col")
    stretches = events // STRETCH
    per = heads // rows
    parts = 1
    pieces = users * per * parts
    total = users * events
    tall = 2 * STRETCH if events % (2 * STRETCH) == 0 else STRETCH
    group = rows * LANES
    head = (state_width // parts, LANES)

    vmem = pl.BlockSpec(memory_space=pltpu.VMEM)
    hbm = pl.BlockSpec(memory_space=pltpu.HBM)
    dma = pltpu.SemaphoreType.DMA

    def f32(*shape):
        return pltpu.VMEM(shape, F32)

    def bf16(*shape):
        return pltpu.VMEM(shape, BF16)

    result = pl.pallas_call(
        functools.partial(mixer_kernel, (rows, cols, users, heads, tall, parts)),
        in_specs=[hbm] * 12,
        out_specs=vmem,
        out_shape=jax.ShapeDtypeStruct((total, w_out.shape[1]), BF16),
        scratch_shapes=[
            pltpu.SMEM(lengths.shape, jnp.int32),
            pltpu.VMEM(item_ids.shape, jnp.int32),
            pltpu.VMEM(pad_masks.shape, jnp.int32),
            bf16(*w_dt.shape[::-1]),
            f32(*conv_taps.shape),
            f32(1, heads),
            f32(1, heads),
            f32(1, inner),
            bf16(items, model),
            bf16(model, full_width),
            bf16(model, inner),
            bf16(*w_out.shape),
            bf16(items, full_width),
            bf16(items, inner),
            bf16(4 * heads, items),
            bf16(2 * heads, model),
            f32(2, heads, LANES),
            f32(heads + 2, 8, LANES),
            bf16(users, HALO + events, items),
            f32(users, heads + 2, HALO + events, LANES),
            bf16(users, state_width, events),
            bf16(total, state_width),
            f32(total, LANES),
            f32(users, stretches, heads, LANES),
            f32(users, stretches, heads, LANES),
            f32(users * per, stretches, 8, group),
            bf16(users, heads, events, LANES),
            bf16(users, per, events, group),
            bf16(users * per, stretches, state_width, group),
            bf16(pieces, rows, *head),
            bf16(pieces, rows, *head),
            f32(users, rows, per, 8, LANES),
            f32(users, rows, per, 8, LANES),
            f32(pieces, rows + 1, *head),
            f32(pieces, rows + 1, 8, LANES),
            f32(*head),
            bf16(pieces, *head),
            bf16(pieces, *head),
            f32(pieces, 8, LANES),
            bf16(pieces, *head),
            bf16(pieces, *head),
            f32(pieces, 8, LANES),
            bf16(pieces, rows, *head),
            bf16(pieces, rows, *head),
            f32(total, inner),
            f32(total, inner),
            bf16(events // tall, tall, group),
            f32(events // tall, tall, LANES),
            f32(events // tall, tall, w_out.shape[1]),
            pltpu.VMEM((users, 1, STRETCH), jnp.int32),
            dma((2 * heads + 4,)),
            dma((8,)),
            dma((2,)),
            dma((users, rows)),
            dma((users, rows)),
            dma((pieces, rows)),
            dma((pieces, rows)),
            dma((pieces,)),
            dma((pieces,)),
            dma((pieces, rows)),
            dma((pieces, rows)),
            dma((pieces,)),
            dma((pieces,)),
            dma((pieces,)),
            dma((pieces,)),
        ],
        compiler_params=pltpu.CompilerParams(
            collective_id=0, has_side_effects=True, vmem_limit_bytes=48 * 1024 * 1024
        ),
        name="mixer",
    )(
        *(
            pltpu.with_memory_space_constraint(array, pltpu.HBM)
            for array in (
                lengths,
                item_ids,
                pad_masks,
                w_dt.T,
                conv_taps,
                dt_bias[None],
                decay_rates[None],
                norm_gain[None],
                item_table,
                w_in,
                w_gate,
                w_out,
            )
        )
    )
    return result.reshape(users, 1, events, -1)


def solution(mesh):
    in_specs = (
        P("batch", "col", "row"),
        P("batch", "col", "row"),
        P("batch"),
        P(),
        P(),
        P(),
        P(),
        P(),
        P(),
        P(),
        P(),
        P(),
    )
    out_specs = P("batch", "col", "row", None)
    return jax.shard_map(
        per_device, mesh=mesh, in_specs=in_specs, out_specs=out_specs, check_vma=False
    )
```
